128 devices in a mesh: tm: 8 (over y, core), ep: 16 (over x, z).
Axes of the slice: x: 4, y: 4, z: 4, core: 2. Of those that a mesh axis runs over, the one named last changes fastest.
Arguments:
- observations: bfloat16 [1024, 128, 1024], P('ep', 'tm'), may hold values from -6 to 6
- input_weight: bfloat16 [1024, 2048], replicated, may hold values from -0.1875 to 0.1875
- hidden_weight: bfloat16 [512, 2048], replicated, may hold values from -0.25 to 0.25
- gate_bias: float32 [2048], replicated, may hold values from -3 to 3
- forget_bias: float32 [512], replicated, may hold values from 0 to 5
- episode_ids: int32 [2048], P('ep'), may hold values from 0 to 63
- start_steps: int32 [2048], P('ep'), may hold values from 0 to 127
- priorities: int32 [2048], P('ep'), may hold values from 20 to 999
Outputs:
- train_rows: bfloat16 [2048, 128, 1024], P('ep', 'tm')
- start_state: bfloat16 [2048, 2, 512], P('ep')
- sample_weights: bfloat16 [2048], P('ep')
The draws below stay inside these ranges and needn't reach their ends.
Inputs may be any that keep to these rules, and one draw needn't show every extreme that they name: `episode_ids`: slot index inside the storage shard that sampled the sequence.
All inputs are finite; a program needn't handle non-finite values.
Results may differ from the reference program's by a relative error of at most 0.009.
Values may be sent and summed in bfloat16 or wider, within the bound.
No kernel may reach another device: no remote copies, remote signals or barrier semaphores. Data moves between devices by JAX's collectives and lax.ppermute only.
A program may use at most 64 MiB of HBM per device.

```python
import jax
import jax.numpy as jnp
from jax import lax

H = 512
OBS = 1024
STEPS = 128
BURN = 40
UNROLL = 80
EPI_DEV = 64
SEQ_COL = 128
EPISODES = 1024
SEQS = 2048
N_EP = 16


def draw_priorities(key, part):
    low_key = jax.random.fold_in(key, 71)
    rest_key = jax.random.fold_in(key, 72)
    place_key = jax.random.fold_in(key, 73)
    lowest = jax.random.randint(low_key, (), 20, 301)
    others = jax.random.randint(rest_key, (SEQS,), 2 * lowest, 1000)
    planted = jax.random.randint(place_key, (), 0, SEQS)
    return others.at[planted].set(lowest).astype(jnp.int32)


def set_ends(entries, rng, low, high):
    place = [jax.random.randint(jax.random.fold_in(rng, axis), (), 0, length) for axis, length in enumerate(entries.shape)]
    longest = entries.shape.index(max(entries.shape))
    next_to = place[:longest] + [(place[longest] + 1) % entries.shape[longest]] + place[longest + 1:]
    return entries.at[tuple(place)].set(low).at[tuple(next_to)].set(high)


def block_scale(key, dims, split, low, high):
    gain = 1.0
    for axis_at, parts in split:
        draws = jax.random.uniform(jax.random.fold_in(jax.random.fold_in(key, 6), axis_at), (parts,), jnp.float32, low / len(split), high / len(split))
        gain = gain * jnp.repeat(jnp.exp(draws), dims[axis_at] // parts).reshape((-1,) + (1,) * (len(dims) - 1 - axis_at))
    return gain


def bell_draw(own_key, dims, spread, bound, cuts=(), kind=jnp.bfloat16):
    entries = spread * jax.random.normal(own_key, dims, jnp.float32)
    if cuts:
        entries = entries * block_scale(own_key, dims, cuts, -0.22, 0.18)
    return jnp.clip(entries, -bound, bound).astype(kind)


def setup_inputs(seed: int = 0) -> dict:
    arg_keys = jax.random.split(jax.random.key(seed), 9)
    return {
        "observations": bell_draw(arg_keys[0], (EPISODES, STEPS, OBS), 1.0, 6.0, ((0, 16), (1, 8))),
        "input_weight": bell_draw(arg_keys[1], (OBS, 4 * H), OBS ** -0.5, 0.1875),
        "hidden_weight": bell_draw(arg_keys[2], (H, 4 * H), H ** -0.5, 0.25),
        "gate_bias": bell_draw(arg_keys[3], (4 * H,), 0.5, 3.0, (), jnp.float32),
        "forget_bias": jnp.clip(jax.random.uniform(arg_keys[4], (H,), jnp.float32, 0.0, 5.0), 0.0, 5.0),
        "episode_ids": set_ends(jax.random.randint(arg_keys[5], (SEQS,), 0, EPI_DEV), jax.random.fold_in(arg_keys[5], 1), 0, EPI_DEV - 1).astype(jnp.int32),
        "start_steps": set_ends(jax.random.randint(arg_keys[6], (SEQS,), 0, STEPS), jax.random.fold_in(arg_keys[6], 1), 0, STEPS - 1).astype(jnp.int32),
        "priorities": draw_priorities(jax.random.fold_in(arg_keys[8], 71), 0),
    }


IMPORTANCE = 0.6


def lstm_step(state_pair, projected, hidden_weight, gate_bias, forget_bias):
    hidden, cell_state = state_pair
    hidden_width = hidden.shape[-1]
    gate_sum = projected + jnp.dot(hidden.astype(jnp.bfloat16), hidden_weight, preferred_element_type=jnp.float32) + gate_bias
    ingate = gate_sum[:, :hidden_width]
    forget = gate_sum[:, hidden_width:2 * hidden_width]
    candidate = gate_sum[:, 2 * hidden_width:3 * hidden_width]
    outgate = gate_sum[:, 3 * hidden_width:]
    cell_state = jax.nn.sigmoid(forget + forget_bias) * cell_state + jax.nn.sigmoid(ingate) * jnp.tanh(candidate)
    hidden = jax.nn.sigmoid(outgate) * jnp.tanh(cell_state)
    return hidden, cell_state


def owner_order(values):
    trailing = values.shape[1:]
    blocked = values.reshape((N_EP, N_EP, SEQ_COL // N_EP) + trailing)
    return jnp.swapaxes(blocked, 0, 1).reshape((SEQS,) + trailing)


def reference(observations, input_weight, hidden_weight, gate_bias, forget_bias, episode_ids, start_steps, priorities):
    sequence = jnp.arange(SEQS, dtype=jnp.int32)
    episode = (sequence // SEQ_COL) * EPI_DEV + episode_ids

    def advance(state_pair, offset):
        step_index = (start_steps + offset) % STEPS
        inputs = observations[episode, step_index]
        projected = jnp.dot(inputs, input_weight, preferred_element_type=jnp.float32)
        return lstm_step(state_pair, projected, hidden_weight, gate_bias, forget_bias), None

    blank_state = jnp.zeros((SEQS, H), jnp.float32)
    (hidden, cell_state), _ = lax.scan(advance, (blank_state, blank_state), jnp.arange(BURN, dtype=jnp.int32))
    start_state = jnp.stack([hidden, cell_state], axis=1).astype(jnp.bfloat16)
    raw_weight = jnp.exp(-IMPORTANCE * jnp.log(priorities.astype(jnp.float32))).astype(jnp.bfloat16)
    peak_weight = jnp.max(raw_weight.astype(jnp.float32))
    weights = (raw_weight.astype(jnp.float32) / peak_weight).astype(jnp.bfloat16)
    offsets = (jnp.arange(STEPS, dtype=jnp.int32)[None, :] - start_steps[:, None] - BURN) % STEPS
    keep_mask = offsets < UNROLL
    masked_rows = jnp.where(keep_mask[:, :, None], observations[episode], jnp.zeros((), jnp.bfloat16))
    return owner_order(masked_rows), owner_order(start_state), owner_order(weights)
```

```python
import functools

import jax
import jax.numpy as jnp
from jax import lax
from jax.experimental import pallas as pl
from jax.experimental.pallas import tpu as pltpu
from jax.sharding import Mesh
from jax.sharding import PartitionSpec as P

STEPS = 128
BURN = 40
UNROLL = 80
SPAN = 4
EP = ("ep_0", "ep_1")
IMPORTANCE = 0.6


def sigmoid(x):
    return 0.5 * jnp.tanh(0.5 * x) + 0.5


def burn_in_kernel(
    starts, x_hbm, win_hbm, wh_hbm, off_ref, bias_ref, out_ref, xs, win, wh, hot, proj, xsem, wsem, hsem
):
    shards, count, rows, _ = x_hbm.shape
    hidden_width = wh.shape[0]
    win_copy = pltpu.make_async_copy(win_hbm, win, wsem)
    wh_copy = pltpu.make_async_copy(wh_hbm, wh, hsem)
    for s in range(count):
        first = starts[s] // rows
        for j in range(SPAN):
            pltpu.make_async_copy(
                x_hbm.at[(first + j) % shards, s],
                xs.at[pl.ds((s * SPAN + j) * rows, rows)],
                xsem,
            ).start()
    win_copy.start()
    wh_copy.start()
    span = SPAN * rows
    column = lax.broadcasted_iota(jnp.int32, (count, count * span), 1)
    sequence = lax.broadcasted_iota(jnp.int32, (count, count * span), 0)
    gap = column - sequence * span - off_ref[...]
    for t in range(BURN):
        hot[t * count : (t + 1) * count, :] = jnp.where(gap == t, 1.0, 0.0).astype(jnp.bfloat16)
    pltpu.make_async_copy(xs, xs, xsem).wait()
    x = jnp.dot(hot[...], xs[...], preferred_element_type=jnp.float32).astype(jnp.bfloat16)
    win_copy.wait()
    proj[...] = jnp.dot(x, win[...], preferred_element_type=jnp.float32) + bias_ref[...]
    wh_copy.wait()

    def step(t, state_pair):
        hidden, cell_state = state_pair
        projected = proj[pl.ds(pl.multiple_of(t * count, count), count), :]
        gate_sum = projected + jnp.dot(hidden, wh[...], preferred_element_type=jnp.float32)
        ingate = sigmoid(gate_sum[:, :hidden_width])
        forget = sigmoid(gate_sum[:, hidden_width : 2 * hidden_width])
        candidate = jnp.tanh(gate_sum[:, 2 * hidden_width : 3 * hidden_width])
        outgate = sigmoid(gate_sum[:, 3 * hidden_width :])
        cell_state = forget * cell_state + ingate * candidate
        return ((outgate * jnp.tanh(cell_state)).astype(jnp.bfloat16), cell_state)

    blank = (
        jnp.zeros((count, hidden_width), jnp.bfloat16),
        jnp.zeros((count, hidden_width), jnp.float32),
    )
    hidden, cell_state = lax.fori_loop(0, BURN, step, blank, unroll=4)
    out_ref[0] = hidden
    out_ref[1] = cell_state.astype(jnp.bfloat16)


def burn_in(starts, x, input_weight, hidden_weight, bias):
    _, count, rows, width = x.shape
    hidden_width = hidden_weight.shape[0]
    hbm = pl.BlockSpec(memory_space=pltpu.HBM)
    vmem = pl.BlockSpec(memory_space=pltpu.VMEM)
    return pl.pallas_call(
        burn_in_kernel,
        out_shape=jax.ShapeDtypeStruct((2, count, hidden_width), jnp.bfloat16),
        in_specs=[pl.BlockSpec(memory_space=pltpu.SMEM), hbm, hbm, hbm, vmem, vmem],
        out_specs=vmem,
        scratch_shapes=[
            pltpu.VMEM((count * SPAN * rows, width), jnp.bfloat16),
            pltpu.VMEM(input_weight.shape, jnp.bfloat16),
            pltpu.VMEM(hidden_weight.shape, jnp.bfloat16),
            pltpu.VMEM((BURN * count, count * SPAN * rows), jnp.bfloat16),
            pltpu.VMEM((BURN * count, 4 * hidden_width), jnp.float32),
            pltpu.SemaphoreType.DMA,
            pltpu.SemaphoreType.DMA,
            pltpu.SemaphoreType.DMA,
        ],
        compiler_params=pltpu.CompilerParams(vmem_limit_bytes=32 * 1024 * 1024),
        cost_estimate=pl.CostEstimate(
            flops=30_000_000_000, bytes_accessed=8 * 1024 * 1024, transcendentals=0
        ),
        name="burn_in",
    )(starts, x, input_weight, hidden_weight, (starts % rows)[:, None], bias)


def body(
    observations,
    input_weight,
    hidden_weight,
    gate_bias,
    forget_bias,
    episode_ids,
    start_steps,
    priorities,
):
    shard_steps, width = observations.shape[1:]
    seq_count = episode_ids.shape[0]
    hidden_width = hidden_weight.shape[0]
    time_shards = lax.axis_size("tm")
    learners = lax.axis_size(EP)
    position = lax.axis_index("tm")
    own_count = seq_count // time_shards
    per_learner = seq_count // learners
    stored_rows = observations[episode_ids]
    slots = lax.all_to_all(stored_rows, "tm", split_axis=0, concat_axis=0, tiled=True)
    slots = slots.reshape(time_shards, own_count, shard_steps, width)

    local_steps = position * shard_steps + jnp.arange(shard_steps, dtype=jnp.int32)
    offsets = (local_steps[None, :] - start_steps[:, None] - BURN) % STEPS
    sent_rows = jnp.where((offsets < UNROLL)[:, :, None], stored_rows, jnp.zeros((), jnp.bfloat16))
    moved_rows = lax.all_to_all(sent_rows, EP, split_axis=0, concat_axis=0, tiled=True)

    own_starts = lax.dynamic_slice_in_dim(start_steps, position * own_count, own_count)
    blank = jnp.zeros((hidden_width,), jnp.float32)
    bias = gate_bias + jnp.concatenate([blank, forget_bias, blank, blank])
    own_pair = burn_in(own_starts, slots, input_weight, hidden_weight, bias[None, :])
    own_pair = jnp.swapaxes(own_pair, 0, 1)

    pairs = lax.all_gather(own_pair, "tm", axis=0, tiled=True)
    pairs = pairs.reshape(learners, per_learner, 2, hidden_width)
    raw_weight = jnp.exp(-IMPORTANCE * jnp.log(priorities.astype(jnp.float32))).astype(jnp.bfloat16)
    peak = jnp.broadcast_to(jnp.max(raw_weight), (learners, 1))
    extra = jnp.concatenate([raw_weight.reshape(learners, per_learner), peak], axis=1)
    extra = jnp.pad(extra, ((0, 0), (0, 2 * hidden_width - per_learner - 1)))
    both = jnp.concatenate([pairs, extra.reshape(learners, 1, 2, hidden_width)], axis=1)
    both = lax.all_to_all(both, EP, split_axis=0, concat_axis=0, tiled=True)
    start_state = both[:, :per_learner].reshape(seq_count, 2, hidden_width)
    extra = both[:, per_learner, 0, : per_learner + 1].astype(jnp.float32)
    weights = (extra[:, :per_learner] / jnp.max(extra[:, per_learner])).astype(jnp.bfloat16)
    return (moved_rows, start_state, weights.reshape(seq_count))


def solution(mesh):
    torus = Mesh(mesh.devices.reshape(mesh.shape["tm"], 4, 4), ("tm", "ep_0", "ep_1"))
    return jax.shard_map(
        body,
        mesh=torus,
        in_specs=(P(EP, "tm", None), P(), P(), P(), P(), P(EP), P(EP), P(EP)),
        out_specs=(P(EP, "tm", None), P(EP, None, None), P(EP)),
        check_vma=False,
    )
```

```python
import functools

import jax
import jax.numpy as jnp
from jax import lax
from jax.experimental import pallas as pl
from jax.experimental.pallas import tpu as pltpu
from jax.sharding import Mesh
from jax.sharding import PartitionSpec as P

STEPS = 128
BURN = 40
UNROLL = 80
ROOM = 128
EP = ("ep_0", "ep_1")
IMPORTANCE = 0.6
MIB = 1024 * 1024
SMEM = pl.BlockSpec(memory_space=pltpu.SMEM)
VMEM = pl.BlockSpec(memory_space=pltpu.VMEM)
HBM = pl.BlockSpec(memory_space=pltpu.HBM)


def sigmoid(x):
    return 0.5 * jnp.tanh(0.5 * x) + 0.5


def iota(shape, dim):
    return lax.broadcasted_iota(jnp.int32, shape, dim)


def one_hot(hit):
    return jnp.where(hit, 1.0, 0.0).astype(jnp.bfloat16)


def f32_dot(a, b):
    return jnp.dot(a, b, preferred_element_type=jnp.float32)


def pack_kernel(base, place, ids, starts_ref, obs, *rest):
    outs, rows_of = rest[:-1], rest[-1]
    shards, count = starts_ref.shape
    shard_steps = obs.shape[1]
    lanes = count * shard_steps
    spread = one_hot(iota((count, lanes), 1) // shard_steps == iota((count, lanes), 0))
    starts = f32_dot(starts_ref[...].astype(jnp.bfloat16), spread).astype(jnp.int32)
    step = place[0] * shard_steps + iota((shards, lanes), 1) % shard_steps
    within = ((step - starts) & (STEPS - 1)) < BURN
    before = one_hot(iota((lanes, lanes), 0) < iota((lanes, lanes), 1))
    slot = f32_dot(one_hot(within), before).astype(jnp.int32) - base
    slot = jnp.where(within, slot, -1)
    for k in range(shards):
        for i in range(count):
            rows_of[k, i * shard_steps : (i + 1) * shard_steps, :] = obs[ids[k, i]]
    for k in range(shards):
        hot = one_hot(iota((ROOM, lanes), 0) == slot[k : k + 1, :])
        outs[k][...] = f32_dot(hot, rows_of[k]).astype(jnp.bfloat16)


def pack(base, position, ids, starts, observations):
    shards, count = ids.shape
    _, shard_steps, width = observations.shape
    return pl.pallas_call(
        functools.partial(pack_kernel, base),
        out_shape=[jax.ShapeDtypeStruct((ROOM, width), jnp.bfloat16)] * shards,
        in_specs=[SMEM, SMEM, VMEM, VMEM],
        out_specs=[VMEM] * shards,
        scratch_shapes=[pltpu.VMEM((shards, count * shard_steps, width), jnp.bfloat16)],
        compiler_params=pltpu.CompilerParams(vmem_limit_bytes=24 * MIB),
        cost_estimate=pl.CostEstimate(flops=10**9, bytes_accessed=4 * MIB, transcendentals=0),
        name="pack_rows",
    )(position.reshape(1), ids, starts, observations)


def masked_kernel(place, ids_hbm, starts_hbm, obs, out, ids, starts, sem):
    block = pl.program_id(0)

    @pl.when(block == 0)
    def _():
        ids_copy = pltpu.make_async_copy(ids_hbm, ids, sem.at[0])
        starts_copy = pltpu.make_async_copy(starts_hbm, starts, sem.at[1])
        ids_copy.start()
        starts_copy.start()
        ids_copy.wait()
        starts_copy.wait()

    count, shard_steps, width = out.shape
    step = place[0] * shard_steps + iota((shard_steps, width), 0)
    for i in range(count):
        g = block * count + i
        keep = ((step - starts[g] - BURN) & (STEPS - 1)) < UNROLL
        out[i] = jnp.where(keep, obs[ids[g]], jnp.zeros((), jnp.bfloat16))


def masked(position, ids, starts, observations):
    _, shard_steps, width = observations.shape
    count = 8
    return pl.pallas_call(
        masked_kernel,
        grid=(ids.shape[0] // count,),
        out_shape=jax.ShapeDtypeStruct((ids.shape[0], shard_steps, width), jnp.bfloat16),
        in_specs=[SMEM, HBM, HBM, VMEM],
        out_specs=pl.BlockSpec((count, shard_steps, width), lambda b: (b, 0, 0)),
        scratch_shapes=[
            pltpu.SMEM(ids.shape, jnp.int32),
            pltpu.SMEM(starts.shape, jnp.int32),
            pltpu.SemaphoreType.DMA((2,)),
        ],
        compiler_params=pltpu.CompilerParams(vmem_limit_bytes=60 * MIB),
        cost_estimate=pl.CostEstimate(flops=10**8, bytes_accessed=6 * MIB, transcendentals=0),
        name="masked_rows",
    )(position.reshape(1), ids, starts, observations)


def copy_kernel(rows, out):
    out[...] = rows[...]


def copied(rows):
    _, shard_steps, width = rows.shape
    block = pl.BlockSpec((16, shard_steps, width), lambda b: (b, 0, 0))
    return pl.pallas_call(
        copy_kernel,
        grid=(rows.shape[0] // 16,),
        out_shape=jax.ShapeDtypeStruct(rows.shape, rows.dtype),
        in_specs=[block],
        out_specs=block,
        compiler_params=pltpu.CompilerParams(vmem_limit_bytes=48 * MIB),
        cost_estimate=pl.CostEstimate(flops=10**9, bytes_accessed=8 * MIB, transcendentals=0),
        name="copy_rows",
    )(rows)


def burn_in_kernel(rounds, *refs):
    parts, refs = refs[: 8 * rounds], refs[8 * rounds :]
    columns, (win_hbm, wh_hbm, bias_ref, out_ref), refs = refs[:rounds], refs[rounds : rounds + 4], refs[rounds + 4 :]
    xs, hots, (win, wh, proj, xsem, wsem, hsem) = refs[:rounds], refs[rounds : 2 * rounds], refs[2 * rounds :]
    copies, _, count, hidden_width = out_ref.shape
    win_copy = pltpu.make_async_copy(win_hbm, win, wsem)
    wh_copy = pltpu.make_async_copy(wh_hbm, wh, hsem)
    row_copies = [
        pltpu.make_async_copy(part, xs[n // 8].at[pl.ds((n % 8) * ROOM, ROOM)], xsem.at[n])
        for n, part in enumerate(parts)
    ]
    for copy in row_copies:
        copy.start()
    win_copy.start()
    wh_copy.start()
    lane = iota((count, 8 * ROOM), 1)
    for hot, column in zip(hots, columns):
        for t in range(BURN):
            at = slice(t * count, (t + 1) * count)
            hot[at, :] = one_hot(lane == column[at, :])
    for copy in row_copies:
        copy.wait()
    x = sum(f32_dot(hot[...], rows[...]) for hot, rows in zip(hots, xs)).astype(jnp.bfloat16)
    win_copy.wait()
    proj[...] = f32_dot(x, win[...]) + bias_ref[...]
    wh_copy.wait()

    half = hidden_width // 2

    def step(t, state_pair):
        hiddens, cells = state_pair
        row = pl.ds(pl.multiple_of(t * count, count), count)
        blocks = [[pl.ds(gate * hidden_width + q * half, half) for gate in range(4)] for q in range(2)]
        sums = [[proj[row, block] for block in part] for part in blocks]
        for k in range(2):
            for q in range(2):
                for gate in range(4):
                    weight = wh[k * half : (k + 1) * half, blocks[q][gate]]
                    sums[q][gate] = sums[q][gate] + f32_dot(hiddens[k], weight)
        new_hiddens, new_cells = [], []
        for (ingate, forget, candidate, outgate), cell_state in zip(sums, cells):
            cell_state = sigmoid(forget) * cell_state + sigmoid(ingate) * jnp.tanh(candidate)
            new_cells.append(cell_state)
            new_hiddens.append((sigmoid(outgate) * jnp.tanh(cell_state)).astype(jnp.bfloat16))
        return (tuple(new_hiddens), tuple(new_cells))

    blank = ((jnp.zeros((count, half), jnp.bfloat16),) * 2, (jnp.zeros((count, half), jnp.float32),) * 2)
    hiddens, cells = lax.fori_loop(0, BURN, step, blank, unroll=8)
    hidden = jnp.concatenate(hiddens, axis=1)
    cell_state = jnp.concatenate(cells, axis=1)
    for n in range(copies):
        out_ref[n, 0] = hidden
        out_ref[n, 1] = cell_state.astype(jnp.bfloat16)


def burn_in(parts, columns, input_weight, hidden_weight, bias):
    rounds = len(columns)
    shards = len(parts) // rounds
    width = input_weight.shape[0]
    hidden_width = hidden_weight.shape[0]
    total = columns[0].shape[0]
    count = total // BURN
    return pl.pallas_call(
        functools.partial(burn_in_kernel, rounds),
        out_shape=jax.ShapeDtypeStruct((shards, 2, count, hidden_width), jnp.bfloat16),
        in_specs=[HBM] * len(parts) + [VMEM] * rounds + [HBM, HBM, VMEM],
        out_specs=VMEM,
        scratch_shapes=[pltpu.VMEM((shards * ROOM, width), jnp.bfloat16)] * rounds
        + [pltpu.VMEM((total, shards * ROOM), jnp.bfloat16)] * rounds
        + [
            pltpu.VMEM(input_weight.shape, jnp.bfloat16),
            pltpu.VMEM(hidden_weight.shape, jnp.bfloat16),
            pltpu.VMEM((total, 4 * hidden_width), jnp.float32),
            pltpu.SemaphoreType.DMA((len(parts),)),
            pltpu.SemaphoreType.DMA,
            pltpu.SemaphoreType.DMA,
        ],
        compiler_params=pltpu.CompilerParams(vmem_limit_bytes=32 * MIB),
        cost_estimate=pl.CostEstimate(
            flops=30_000_000_000, bytes_accessed=8 * MIB, transcendentals=0
        ),
        name="burn_in",
    )(*parts, *columns, input_weight, hidden_weight, bias)


def order_kernel(pairs, rank, raw, out):
    shards, _, count, hidden_width = pairs.shape
    total = shards * count
    column = iota((total, total), 1)
    hot = one_hot((column % count) * shards + column // count == rank[...])
    for n in range(2):
        state = pairs[:, n].reshape(total, hidden_width)
        out[:, n * hidden_width : (n + 1) * hidden_width] = f32_dot(hot, state).astype(jnp.bfloat16)
    lane = iota((total, 128), 1)
    tail = jnp.where(lane == 0, raw[...], jnp.where(lane == 1, jnp.max(raw[...]), 0.0))
    out[:, 2 * hidden_width :] = tail.astype(jnp.bfloat16)


def ordered(pairs, rank, raw):
    total = rank.shape[0]
    return pl.pallas_call(
        order_kernel,
        out_shape=jax.ShapeDtypeStruct((total, 2 * pairs.shape[3] + 128), jnp.bfloat16),
        in_specs=[VMEM] * 3,
        out_specs=VMEM,
        compiler_params=pltpu.CompilerParams(vmem_limit_bytes=8 * MIB),
        cost_estimate=pl.CostEstimate(flops=10**8, bytes_accessed=MIB, transcendentals=0),
        name="learner_order",
    )(pairs, rank[:, None], raw[:, None])


def rows_in_shard(starts, shard, shard_steps):
    part = (shard - starts // shard_steps) % (STEPS // shard_steps)
    first = part * shard_steps - starts % shard_steps
    return jnp.clip(jnp.minimum(BURN, first + shard_steps) - jnp.maximum(first, 0), 0, shard_steps)


def body(
    observations,
    input_weight,
    hidden_weight,
    gate_bias,
    forget_bias,
    episode_ids,
    start_steps,
    priorities,
):
    shard_steps, _ = observations.shape[1:]
    seq_count = episode_ids.shape[0]
    hidden_width = hidden_weight.shape[0]
    shards = lax.axis_size("tm")
    learners = lax.axis_size(EP)
    position = lax.axis_index("tm").astype(jnp.int32)
    own_count = seq_count // shards
    per_learner = seq_count // learners

    index = jnp.arange(seq_count, dtype=jnp.int32)
    key = start_steps * seq_count + index
    rank = jnp.sum((key[None, :] < key[:, None]).astype(jnp.int32), axis=1)
    turn = jnp.arange(shards, dtype=jnp.int32)
    dealt = jnp.arange(own_count, dtype=jnp.int32)[None, :] * shards + ((position + turn) % shards)[:, None]
    chosen = rank[None, None, :] == dealt[:, :, None]
    ids = jnp.sum(jnp.where(chosen, episode_ids, 0), axis=2)
    starts = jnp.sum(jnp.where(chosen, start_steps, 0), axis=2)

    def exchanged(base):
        sent = pack(base, position, ids, starts, observations)
        parts = [sent[0]]
        for k in range(1, shards):
            ring = [(i, (i + k) % shards) for i in range(shards)]
            parts.append(lax.ppermute(sent[k], "tm", ring))
        return parts

    parts = exchanged(0)
    sent_rows = masked(position, episode_ids, start_steps, observations)
    moved_rows = lax.all_to_all(sent_rows, EP, split_axis=0, concat_axis=0, tiled=True)

    own = starts[0]
    step = jnp.arange(BURN, dtype=jnp.int32)[:, None]
    shard = (own + step) % STEPS // shard_steps
    earlier = jnp.arange(own_count)[None, None, :] < jnp.arange(own_count)[None, :, None]
    ahead = jnp.sum(
        jnp.where(earlier, rows_in_shard(own[None, None, :], shard[:, :, None], shard_steps), 0), axis=2
    )
    first = jnp.maximum((own % shard_steps + step) // shard_steps * shard_steps - own % shard_steps, 0)
    slot = ahead + step - first
    sender = (position - shard) % shards
    column = (sender * ROOM + slot % ROOM).reshape(BURN * own_count, 1)
    late = (slot >= ROOM).reshape(BURN * own_count, 1)
    pair_rows = jnp.sum(rows_in_shard(starts[None], turn[:, None, None], shard_steps), axis=2)
    crowded = jnp.max(pair_rows) > ROOM

    blank = jnp.zeros((hidden_width,), jnp.float32)
    bias = (gate_bias + jnp.concatenate([blank, forget_bias, blank, blank]))[None, :]

    def usual():
        return burn_in(parts, [column], input_weight, hidden_weight, bias)

    def two_rounds():
        columns = [jnp.where(late, -1, column), jnp.where(late, column, -1)]
        more = exchanged(ROOM)
        return burn_in(parts + more, columns, input_weight, hidden_weight, bias)

    pairs = lax.cond(crowded, two_rounds, usual)
    pairs, moved_rows = lax.optimization_barrier((pairs, moved_rows))
    pairs = lax.all_to_all(pairs, "tm", split_axis=0, concat_axis=0, tiled=True)
    moved_rows = copied(moved_rows)
    raw_weight = jnp.exp(-IMPORTANCE * jnp.log(priorities.astype(jnp.float32))).astype(jnp.bfloat16)
    both = ordered(pairs, rank, raw_weight.astype(jnp.float32))
    both = both.reshape(learners, per_learner, both.shape[1])
    both = lax.all_to_all(both, EP, split_axis=0, concat_axis=0, tiled=True)
    start_state = both[:, :, : 2 * hidden_width].reshape(seq_count, 2, hidden_width)
    raw = both[:, :, 2 * hidden_width].astype(jnp.float32)
    peak = jnp.max(both[:, :, 2 * hidden_width + 1]).astype(jnp.float32)
    weights = (raw / peak).astype(jnp.bfloat16)
    return (moved_rows, start_state, weights.reshape(seq_count))


def solution(mesh):
    torus = Mesh(mesh.devices.reshape(mesh.shape["tm"], 4, 4), ("tm", "ep_0", "ep_1"))
    return jax.shard_map(
        body,
        mesh=torus,
        in_specs=(P(EP, "tm", None), P(), P(), P(), P(), P(EP), P(EP), P(EP)),
        out_specs=(P(EP, "tm", None), P(EP, None, None), P(EP)),
        check_vma=False,
    )
```

```python
import functools

import jax
import jax.numpy as jnp
from jax import lax
from jax.experimental import pallas as pl
from jax.experimental.pallas import tpu as pltpu
from jax.sharding import Mesh
from jax.sharding import PartitionSpec as P

STEPS = 128
BURN = 40
UNROLL = 80
ROOM = 128
EP = ("ep_0", "ep_1")
IMPORTANCE = 0.6
MIB = 1024 * 1024
SMEM = pl.BlockSpec(memory_space=pltpu.SMEM)
VMEM = pl.BlockSpec(memory_space=pltpu.VMEM)
HBM = pl.BlockSpec(memory_space=pltpu.HBM)


def sigmoid(x):
    return 0.5 * jnp.tanh(0.5 * x) + 0.5


def iota(shape, dim):
    return lax.broadcasted_iota(jnp.int32, shape, dim)


def one_hot(hit):
    return jnp.where(hit, 1.0, 0.0).astype(jnp.bfloat16)


def f32_dot(a, b):
    return jnp.dot(a, b, preferred_element_type=jnp.float32)


def pack_kernel(base, place, ids, starts_ref, obs, out, rows_of, packed, sem):
    shards, count = starts_ref.shape
    shard_steps = obs.shape[1]
    lanes = count * shard_steps
    spread = one_hot(iota((count, lanes), 1) // shard_steps == iota((count, lanes), 0))
    starts = f32_dot(starts_ref[...].astype(jnp.bfloat16), spread).astype(jnp.int32)
    step = place[0] * shard_steps + iota((shards, lanes), 1) % shard_steps
    within = ((step - starts) & (STEPS - 1)) < BURN
    before = one_hot(iota((lanes, lanes), 0) < iota((lanes, lanes), 1))
    slot = f32_dot(one_hot(within), before).astype(jnp.int32) - base
    slot = jnp.where(within, slot, -1)
    for k in range(shards):
        for i in range(count):
            rows_of[k, i * shard_steps : (i + 1) * shard_steps, :] = obs[ids[k, i]]
        hot = one_hot(iota((ROOM, lanes), 0) == slot[k : k + 1, :])
        packed[k] = f32_dot(hot, rows_of[k]).astype(jnp.bfloat16)
        pltpu.make_async_copy(packed.at[k], out.at[k], sem.at[k]).start()
    for k in range(shards):
        pltpu.make_async_copy(packed.at[k], out.at[k], sem.at[k]).wait()


def pack(base, position, ids, starts, observations):
    shards, count = ids.shape
    _, shard_steps, width = observations.shape
    return pl.pallas_call(
        functools.partial(pack_kernel, base),
        out_shape=jax.ShapeDtypeStruct((shards, ROOM, width), jnp.bfloat16),
        in_specs=[SMEM, SMEM, VMEM, VMEM],
        out_specs=HBM,
        scratch_shapes=[
            pltpu.VMEM((shards, count * shard_steps, width), jnp.bfloat16),
            pltpu.VMEM((shards, ROOM, width), jnp.bfloat16),
            pltpu.SemaphoreType.DMA((shards,)),
        ],
        compiler_params=pltpu.CompilerParams(vmem_limit_bytes=24 * MIB),
        cost_estimate=pl.CostEstimate(flops=10**9, bytes_accessed=4 * MIB, transcendentals=0),
        name="pack_rows",
    )(position.reshape(1), ids, starts, observations)


def masked_kernel(place, blocks, ids, starts, obs, *refs):
    outs, (held, sem) = refs[:-2], refs[-2:]
    count, shard_steps, width = outs[0].shape
    step = place[0] * shard_steps + iota((shard_steps, width), 0)
    copies = [pltpu.make_async_copy(held.at[n], out, sem.at[n]) for n, out in enumerate(outs)]
    for n in range(len(outs)):
        for i in range(count):
            g = blocks[n] * count + i
            keep = ((step - starts[g] - BURN) & (STEPS - 1)) < UNROLL
            held[n, i] = jnp.where(keep, obs[ids[g]], jnp.zeros((), jnp.bfloat16))
        copies[n].start()
    for copy in copies:
        copy.wait()


def masked(position, blocks, ids, starts, observations):
    _, shard_steps, width = observations.shape
    learners = blocks.shape[0]
    block = (ids.shape[0] // learners, shard_steps, width)
    return pl.pallas_call(
        masked_kernel,
        out_shape=[jax.ShapeDtypeStruct(block, jnp.bfloat16)] * learners,
        in_specs=[SMEM, SMEM, SMEM, SMEM, VMEM],
        out_specs=[HBM] * learners,
        scratch_shapes=[
            pltpu.VMEM((learners, *block), jnp.bfloat16),
            pltpu.SemaphoreType.DMA((learners,)),
        ],
        compiler_params=pltpu.CompilerParams(vmem_limit_bytes=60 * MIB),
        cost_estimate=pl.CostEstimate(flops=10**8, bytes_accessed=6 * MIB, transcendentals=0),
        name="masked_rows",
    )(position.reshape(1), blocks, ids, starts, observations)


def place_kernel(blocks, *refs):
    rows, (out, sem) = refs[:-2], refs[-2:]
    count = rows[0].shape[0]
    copies = [
        pltpu.make_async_copy(block, out.at[pl.ds(blocks[n] * count, count)], sem.at[n])
        for n, block in enumerate(rows)
    ]
    for copy in copies:
        copy.start()
    for copy in copies:
        copy.wait()


def placed(rows, blocks):
    count, shard_steps, width = rows[0].shape
    return pl.pallas_call(
        place_kernel,
        out_shape=jax.ShapeDtypeStruct((len(rows) * count, shard_steps, width), rows[0].dtype),
        in_specs=[SMEM] + [VMEM] * len(rows),
        out_specs=HBM,
        scratch_shapes=[pltpu.SemaphoreType.DMA((len(rows),))],
        compiler_params=pltpu.CompilerParams(vmem_limit_bytes=8 * MIB),
        cost_estimate=pl.CostEstimate(flops=10**9, bytes_accessed=8 * MIB, transcendentals=0),
        name="place_rows",
    )(blocks, *rows)


def burn_in_kernel(rounds, *refs):
    parts, refs = refs[:rounds], refs[rounds:]
    columns, (win_hbm, wh_hbm, bias_ref, out_ref), refs = refs[:rounds], refs[rounds : rounds + 4], refs[rounds + 4 :]
    xs, hots, (win, wh, proj, xsem, wsem, hsem) = refs[:rounds], refs[rounds : 2 * rounds], refs[2 * rounds :]
    copies, _, count, hidden_width = out_ref.shape
    win_copy = pltpu.make_async_copy(win_hbm, win, wsem)
    wh_copy = pltpu.make_async_copy(wh_hbm, wh, hsem)
    row_copies = [
        pltpu.make_async_copy(part, rows, xsem.at[n]) for n, (part, rows) in enumerate(zip(parts, xs))
    ]
    for copy in row_copies:
        copy.start()
    win_copy.start()
    wh_copy.start()
    lane = iota((count, xs[0].shape[0]), 1)
    for hot, column in zip(hots, columns):
        for t in range(BURN):
            at = slice(t * count, (t + 1) * count)
            hot[at, :] = one_hot(lane == column[at, :])
    for copy in row_copies:
        copy.wait()
    x = sum(f32_dot(hot[...], rows[...]) for hot, rows in zip(hots, xs)).astype(jnp.bfloat16)
    win_copy.wait()
    proj[...] = f32_dot(x, win[...]) + bias_ref[...]
    wh_copy.wait()

    half = hidden_width // 2

    def step(t, state_pair):
        hiddens, cells = state_pair
        row = pl.ds(pl.multiple_of(t * count, count), count)
        blocks = [[pl.ds(gate * hidden_width + q * half, half) for gate in range(4)] for q in range(2)]
        sums = [[proj[row, block] for block in part] for part in blocks]
        for k in range(2):
            for q in range(2):
                for gate in range(4):
                    weight = wh[k * half : (k + 1) * half, blocks[q][gate]]
                    sums[q][gate] = sums[q][gate] + f32_dot(hiddens[k], weight)
        new_hiddens, new_cells = [], []
        for (ingate, forget, candidate, outgate), cell_state in zip(sums, cells):
            cell_state = sigmoid(forget) * cell_state + sigmoid(ingate) * jnp.tanh(candidate)
            new_cells.append(cell_state)
            new_hiddens.append((sigmoid(outgate) * jnp.tanh(cell_state)).astype(jnp.bfloat16))
        return (tuple(new_hiddens), tuple(new_cells))

    blank = ((jnp.zeros((count, half), jnp.bfloat16),) * 2, (jnp.zeros((count, half), jnp.float32),) * 2)
    hiddens, cells = lax.fori_loop(0, BURN, step, blank, unroll=8)
    hidden = jnp.concatenate(hiddens, axis=1)
    cell_state = jnp.concatenate(cells, axis=1)
    for n in range(copies):
        out_ref[n, 0] = hidden
        out_ref[n, 1] = cell_state.astype(jnp.bfloat16)


def burn_in(parts, columns, input_weight, hidden_weight, bias):
    rounds = len(columns)
    shards = parts[0].shape[0] // ROOM
    width = input_weight.shape[0]
    hidden_width = hidden_weight.shape[0]
    total = columns[0].shape[0]
    count = total // BURN
    return pl.pallas_call(
        functools.partial(burn_in_kernel, rounds),
        out_shape=jax.ShapeDtypeStruct((shards, 2, count, hidden_width), jnp.bfloat16),
        in_specs=[HBM] * len(parts) + [VMEM] * rounds + [HBM, HBM, VMEM],
        out_specs=VMEM,
        scratch_shapes=[pltpu.VMEM((shards * ROOM, width), jnp.bfloat16)] * rounds
        + [pltpu.VMEM((total, shards * ROOM), jnp.bfloat16)] * rounds
        + [
            pltpu.VMEM(input_weight.shape, jnp.bfloat16),
            pltpu.VMEM(hidden_weight.shape, jnp.bfloat16),
            pltpu.VMEM((total, 4 * hidden_width), jnp.float32),
            pltpu.SemaphoreType.DMA((len(parts),)),
            pltpu.SemaphoreType.DMA,
            pltpu.SemaphoreType.DMA,
        ],
        compiler_params=pltpu.CompilerParams(vmem_limit_bytes=32 * MIB),
        cost_estimate=pl.CostEstimate(
            flops=30_000_000_000, bytes_accessed=8 * MIB, transcendentals=0
        ),
        name="burn_in",
    )(*parts, *columns, input_weight, hidden_weight, bias)


def order_kernel(pairs, rank, raw, out):
    shards, _, count, hidden_width = pairs.shape
    total = shards * count
    column = iota((total, total), 1)
    hot = one_hot((column % count) * shards + column // count == rank[...])
    for n in range(2):
        state = pairs[:, n].reshape(total, hidden_width)
        out[:, n * hidden_width : (n + 1) * hidden_width] = f32_dot(hot, state).astype(jnp.bfloat16)
    lane = iota((total, 128), 1)
    tail = jnp.where(lane == 0, raw[...], jnp.where(lane == 1, jnp.max(raw[...]), 0.0))
    out[:, 2 * hidden_width :] = tail.astype(jnp.bfloat16)


def ordered(pairs, rank, raw):
    total = rank.shape[0]
    return pl.pallas_call(
        order_kernel,
        out_shape=jax.ShapeDtypeStruct((total, 2 * pairs.shape[3] + 128), jnp.bfloat16),
        in_specs=[VMEM] * 3,
        out_specs=VMEM,
        compiler_params=pltpu.CompilerParams(vmem_limit_bytes=8 * MIB),
        cost_estimate=pl.CostEstimate(flops=10**8, bytes_accessed=MIB, transcendentals=0),
        name="learner_order",
    )(pairs, rank, raw)


def weights_kernel(received, out):
    total = received.shape[0]
    raw = received[...].astype(jnp.float32)
    lane = iota(raw.shape, 1)
    peak = jnp.max(jnp.where(lane == 1, raw, 0.0))
    weight = jnp.sum(jnp.where(lane == 0, raw, 0.0), axis=1, keepdims=True) / peak
    weight = jnp.where(iota((total, total), 0) == iota((total, total), 1), weight, 0.0)
    out[...] = jnp.sum(weight, axis=0, keepdims=True).astype(jnp.bfloat16)


def normalized(received):
    total, lanes = received.shape
    return pl.pallas_call(
        weights_kernel,
        grid=(1,),
        out_shape=jax.ShapeDtypeStruct((1, total), jnp.bfloat16),
        in_specs=[pl.BlockSpec((total, 128), lambda n: (0, lanes // 128 - 1))],
        out_specs=pl.BlockSpec((1, total), lambda n: (0, 0)),
        compiler_params=pltpu.CompilerParams(vmem_limit_bytes=4 * MIB),
        name="weights",
    )(received)[0]


def rows_in_shard(starts, shard, shard_steps):
    part = (shard - starts // shard_steps) % (STEPS // shard_steps)
    first = part * shard_steps - starts % shard_steps
    return jnp.clip(jnp.minimum(BURN, first + shard_steps) - jnp.maximum(first, 0), 0, shard_steps)


def body(
    observations,
    input_weight,
    hidden_weight,
    gate_bias,
    forget_bias,
    episode_ids,
    start_steps,
    priorities,
):
    shard_steps, width = observations.shape[1:]
    seq_count = episode_ids.shape[0]
    hidden_width = hidden_weight.shape[0]
    shards = lax.axis_size("tm")
    learners = lax.axis_size(EP)
    position = lax.axis_index("tm").astype(jnp.int32)
    own_count = seq_count // shards
    per_learner = seq_count // learners

    index = jnp.arange(seq_count, dtype=jnp.int32)
    key = start_steps * seq_count + index
    rank = jnp.sum((key[None, :] < key[:, None]).astype(jnp.int32), axis=1)
    turn = jnp.arange(shards, dtype=jnp.int32)
    dealt = jnp.arange(own_count, dtype=jnp.int32)[None, :] * shards + turn[:, None]
    chosen = rank[None, None, :] == dealt[:, :, None]
    ids = jnp.sum(jnp.where(chosen, episode_ids, 0), axis=2)
    starts = jnp.sum(jnp.where(chosen, start_steps, 0), axis=2)

    def exchanged(base):
        sent = pack(base, position, ids, starts, observations)
        rows = lax.all_to_all(sent, "tm", split_axis=0, concat_axis=0, tiled=True)
        return rows.reshape(shards * ROOM, width)

    along, across = lax.axis_size("ep_0"), lax.axis_size("ep_1")
    offsets = jnp.arange(learners, dtype=jnp.int32)
    here = [lax.axis_index(axis).astype(jnp.int32) for axis in EP]

    def block_at(sign):
        first = (here[0] + sign * (offsets // across)) % along
        return first * across + (here[1] + sign * (offsets % across)) % across

    rows_in = exchanged(0)
    sent_rows = masked(position, block_at(1), episode_ids, start_steps, observations)
    moved_rows = [sent_rows[0]]
    for n in range(1, learners):
        ring = [
            (i, (i // across + n // across) % along * across + (i + n) % across)
            for i in range(learners)
        ]
        moved_rows.append(lax.ppermute(sent_rows[n], EP, ring))

    own = lax.dynamic_index_in_dim(starts, position, 0, keepdims=False)
    step = jnp.arange(BURN, dtype=jnp.int32)[:, None]
    shard = (own + step) % STEPS // shard_steps
    earlier = jnp.arange(own_count)[None, None, :] < jnp.arange(own_count)[None, :, None]
    ahead = jnp.sum(
        jnp.where(earlier, rows_in_shard(own[None, None, :], shard[:, :, None], shard_steps), 0), axis=2
    )
    first = jnp.maximum((own % shard_steps + step) // shard_steps * shard_steps - own % shard_steps, 0)
    slot = ahead + step - first
    column = (shard * ROOM + slot % ROOM).reshape(BURN * own_count, 1)
    second = (slot >= ROOM).reshape(BURN * own_count, 1)
    pair_rows = jnp.sum(rows_in_shard(starts[None], turn[:, None, None], shard_steps), axis=2)
    crowded = jnp.max(pair_rows) > ROOM

    blank = jnp.zeros((hidden_width,), jnp.float32)
    bias = (gate_bias + jnp.concatenate([blank, forget_bias, blank, blank]))[None, :]

    raw_weight = jnp.exp(-IMPORTANCE * jnp.log(priorities.astype(jnp.float32))).astype(jnp.bfloat16)
    raw_column = raw_weight.astype(jnp.float32)[:, None]
    column, rank_column, raw_column = lax.optimization_barrier((column, rank[:, None], raw_column))

    def usual():
        return burn_in([rows_in], [column], input_weight, hidden_weight, bias)

    def two_rounds():
        columns = [jnp.where(second, -1, column), jnp.where(second, column, -1)]
        return burn_in([rows_in, exchanged(ROOM)], columns, input_weight, hidden_weight, bias)

    pairs = lax.cond(crowded, two_rounds, usual)
    pairs = lax.all_to_all(pairs, "tm", split_axis=0, concat_axis=0, tiled=True)
    moved_rows = placed(moved_rows, block_at(-1))
    both = ordered(pairs, rank_column, raw_column)
    both = both.reshape(learners, per_learner, both.shape[1])
    both = lax.all_to_all(both, EP, split_axis=0, concat_axis=0, tiled=True)
    start_state = both[:, :, : 2 * hidden_width].reshape(seq_count, 2, hidden_width)
    weights = normalized(both.reshape(seq_count, both.shape[2]))
    return (moved_rows, start_state, weights)


def solution(mesh):
    torus = Mesh(mesh.devices.reshape(mesh.shape["tm"], 4, 4), ("tm", "ep_0", "ep_1"))
    return jax.shard_map(
        body,
        mesh=torus,
        in_specs=(P(EP, "tm", None), P(), P(), P(), P(), P(EP), P(EP), P(EP)),
        out_specs=(P(EP, "tm", None), P(EP, None, None), P(EP)),
        check_vma=False,
    )
```

```python
import functools

import jax
import jax.numpy as jnp
from jax import lax
from jax.experimental import pallas as pl
from jax.experimental.pallas import tpu as pltpu
from jax.sharding import Mesh
from jax.sharding import PartitionSpec as P

STEPS = 128
BURN = 40
UNROLL = 80
ROOM = 128
EP = ("ep_0", "ep_1")
IMPORTANCE = 0.6
MIB = 1024 * 1024
SMEM = pl.BlockSpec(memory_space=pltpu.SMEM)
VMEM = pl.BlockSpec(memory_space=pltpu.VMEM)
HBM = pl.BlockSpec(memory_space=pltpu.HBM)


def sigmoid(x):
    return 0.5 * jnp.tanh(0.5 * x) + 0.5


def iota(shape, dim):
    return lax.broadcasted_iota(jnp.int32, shape, dim)


def one_hot(hit):
    return jnp.where(hit, 1.0, 0.0).astype(jnp.bfloat16)


def f32_dot(a, b):
    return jnp.dot(a, b, preferred_element_type=jnp.float32)


def pack_kernel(base, place, ids, starts_ref, obs, out, crowded, rows_of, packed, sem):
    shards, count = starts_ref.shape
    shard_steps = obs.shape[1]
    lanes = count * shard_steps
    spread = one_hot(iota((count, lanes), 1) // shard_steps == iota((count, lanes), 0))
    starts = f32_dot(starts_ref[...].astype(jnp.bfloat16), spread).astype(jnp.int32)
    step = place[0] * shard_steps + iota((shards, lanes), 1) % shard_steps
    within = ((step - starts) & (STEPS - 1)) < BURN
    before = one_hot(iota((lanes, lanes), 0) < iota((lanes, lanes), 1))
    slot = f32_dot(one_hot(within), before).astype(jnp.int32) - base
    slot = jnp.where(within, slot, -1)
    for k in range(shards):
        for i in range(count):
            rows_of[k, i * shard_steps : (i + 1) * shard_steps, :] = obs[ids[k, i]]
        hot = one_hot(iota((ROOM, lanes), 0) == slot[k : k + 1, :])
        packed[k] = f32_dot(hot, rows_of[k]).astype(jnp.bfloat16)
        pltpu.make_async_copy(packed.at[k], out.at[k], sem.at[k]).start()
    most = jnp.zeros((shards, lanes // 2), jnp.float32)
    for shard in range(shards):
        held = ((step + (shard * shard_steps) - starts) & (STEPS - 1)) < BURN
        some = jnp.where(held, 1.0, 0.0)
        most = jnp.maximum(most, f32_dot(some.astype(jnp.bfloat16), jnp.ones((lanes, lanes // 2), jnp.bfloat16)))
    crowded[0] = (jnp.max(most) > ROOM).astype(jnp.int32)
    for k in range(shards):
        pltpu.make_async_copy(packed.at[k], out.at[k], sem.at[k]).wait()


def pack(base, place, ids, starts, observations):
    shards, count = ids.shape
    _, shard_steps, width = observations.shape
    return pl.pallas_call(
        functools.partial(pack_kernel, base),
        out_shape=(
            jax.ShapeDtypeStruct((shards, ROOM, width), jnp.bfloat16),
            jax.ShapeDtypeStruct((1,), jnp.int32),
        ),
        in_specs=[SMEM, SMEM, VMEM, VMEM],
        out_specs=(HBM, SMEM),
        scratch_shapes=[
            pltpu.VMEM((shards, count * shard_steps, width), jnp.bfloat16),
            pltpu.VMEM((shards, ROOM, width), jnp.bfloat16),
            pltpu.SemaphoreType.DMA((shards,)),
        ],
        compiler_params=pltpu.CompilerParams(vmem_limit_bytes=24 * MIB),
        cost_estimate=pl.CostEstimate(flops=10**9, bytes_accessed=4 * MIB, transcendentals=0),
        name="pack_rows",
    )(place, ids, starts, observations)


def block_at(here, grid, n, sign):
    along, across = grid
    first = lax.rem(here[1] + (along + sign * (n // across)), along)
    return first * across + lax.rem(here[2] + (across + sign * (n % across)), across)


def masked_kernel(grid, place, ids, starts, obs, *refs):
    outs, (held, sem) = refs[:-2], refs[-2:]
    count, shard_steps, width = outs[0].shape
    step = place[0] * shard_steps + iota((shard_steps, width), 0)
    copies = [pltpu.make_async_copy(held.at[n], out, sem.at[n]) for n, out in enumerate(outs)]
    for n in range(len(outs)):
        block = block_at(place, grid, n, 1)
        for i in range(count):
            g = block * count + i
            keep = ((step - starts[g] - BURN) & (STEPS - 1)) < UNROLL
            held[n, i] = jnp.where(keep, obs[ids[g]], jnp.zeros((), jnp.bfloat16))
        copies[n].start()
    for copy in copies:
        copy.wait()


def masked(grid, place, ids, starts, observations):
    _, shard_steps, width = observations.shape
    learners = grid[0] * grid[1]
    block = (ids.shape[0] // learners, shard_steps, width)
    return pl.pallas_call(
        functools.partial(masked_kernel, grid),
        out_shape=[jax.ShapeDtypeStruct(block, jnp.bfloat16)] * learners,
        in_specs=[SMEM, SMEM, SMEM, VMEM],
        out_specs=[HBM] * learners,
        scratch_shapes=[
            pltpu.VMEM((learners, *block), jnp.bfloat16),
            pltpu.SemaphoreType.DMA((learners,)),
        ],
        compiler_params=pltpu.CompilerParams(vmem_limit_bytes=60 * MIB),
        cost_estimate=pl.CostEstimate(flops=10**8, bytes_accessed=6 * MIB, transcendentals=0),
        name="masked_rows",
    )(place, ids, starts, observations)


def place_kernel(grid, sources, place, *refs):
    rows, (out, sem) = refs[: len(sources)], refs[-2:]
    count = rows[0].shape[0]
    copies = [
        pltpu.make_async_copy(
            block, out.at[pl.ds(block_at(place, grid, n, -1) * count, count)], sem.at[m]
        )
        for m, (n, block) in enumerate(zip(sources, rows))
    ]
    for copy in copies:
        copy.start()
    for copy in copies:
        copy.wait()


def placed(grid, sources, place, rows):
    count, shard_steps, width = rows[0].shape
    return pl.pallas_call(
        functools.partial(place_kernel, grid, sources),
        out_shape=jax.ShapeDtypeStruct((grid[0] * grid[1] * count, shard_steps, width), jnp.bfloat16),
        in_specs=[SMEM] + [VMEM] * len(rows),
        out_specs=HBM,
        scratch_shapes=[pltpu.SemaphoreType.DMA((len(rows),))],
        compiler_params=pltpu.CompilerParams(vmem_limit_bytes=8 * MIB),
        cost_estimate=pl.CostEstimate(flops=10**9, bytes_accessed=8 * MIB, transcendentals=0),
        name="place_rows",
    )(place, *rows)


def burn_in_kernel(
    place, crowded, rows_hbm, more_hbm, win_hbm, wh_hbm, bias_ref, starts_ref, out_ref, xs, hot, x, proj, win, wh, pair, sem, out_sem
):
    copies, _, count, hidden_width = out_ref.shape
    shards = starts_ref.shape[0]
    shard_steps = STEPS // shards
    rows_copy = pltpu.make_async_copy(rows_hbm, xs, sem.at[0])
    rows_copy.start()
    win_copy = pltpu.make_async_copy(win_hbm, win, sem.at[2])
    wh_copy = pltpu.make_async_copy(wh_hbm, wh, sem.at[3])
    win_copy.start()
    wh_copy.start()

    mine = jnp.where(iota((shards, count), 0) == place[0], starts_ref[...], 0).astype(jnp.float32)
    mine = jnp.sum(mine, axis=0, keepdims=True)
    diagonal = iota((count, count), 0) == iota((count, count), 1)
    own = jnp.sum(jnp.where(diagonal, mine, 0.0), axis=1, keepdims=True).astype(jnp.int32)
    lane = iota((count, 128), 1)
    first = ((lane - own // shard_steps) & (shards - 1)) * shard_steps - own % shard_steps
    begin = jnp.maximum(first, 0)
    held = jnp.clip(jnp.minimum(first + shard_steps, BURN) - begin, 0, shard_steps)
    earlier = one_hot(iota((count, count), 1) < iota((count, count), 0))
    ahead = f32_dot(earlier, held.astype(jnp.float32).astype(jnp.bfloat16)).astype(jnp.int32)
    slot = iota((count, ROOM), 1)

    def select(base):
        for shard in range(shards):
            at = slice(shard, shard + 1)
            order = slot + base - ahead[:, at]
            step = jnp.where((order >= 0) & (order < held[:, at]), order + begin[:, at], -1)
            for t in range(BURN):
                hot[t * count : (t + 1) * count, shard * ROOM : (shard + 1) * ROOM] = one_hot(step == t)

    select(0)
    rows_copy.wait()
    x[...] = f32_dot(hot[...], xs[...]).astype(jnp.bfloat16)

    @pl.when(crowded[0] > 0)
    def _():
        more_copy = pltpu.make_async_copy(more_hbm, xs, sem.at[1])
        more_copy.start()
        select(ROOM)
        more_copy.wait()
        x[...] += f32_dot(hot[...], xs[...]).astype(jnp.bfloat16)

    win_copy.wait()
    proj[...] = f32_dot(x[...], win[...]) + bias_ref[...]
    wh_copy.wait()
    half = hidden_width // 2

    def step(t, state_pair):
        hiddens, cells = state_pair
        row = pl.ds(pl.multiple_of(t * count, count), count)
        blocks = [[pl.ds(gate * hidden_width + q * half, half) for gate in range(4)] for q in range(2)]
        sums = [[proj[row, block] for block in part] for part in blocks]
        for k in range(2):
            for q in range(2):
                for gate in range(4):
                    weight = wh[k * half : (k + 1) * half, blocks[q][gate]]
                    sums[q][gate] = sums[q][gate] + f32_dot(hiddens[k], weight)
        new_hiddens, new_cells = [], []
        for (ingate, forget, candidate, outgate), cell_state in zip(sums, cells):
            cell_state = sigmoid(forget) * cell_state + sigmoid(ingate) * jnp.tanh(candidate)
            new_cells.append(cell_state)
            new_hiddens.append((sigmoid(outgate) * jnp.tanh(cell_state)).astype(jnp.bfloat16))
        return (tuple(new_hiddens), tuple(new_cells))

    blank = ((jnp.zeros((count, half), jnp.bfloat16),) * 2, (jnp.zeros((count, half), jnp.float32),) * 2)
    hiddens, cells = lax.fori_loop(0, BURN, step, blank, unroll=8)
    pair[0] = jnp.concatenate(hiddens, axis=1)
    pair[1] = jnp.concatenate(cells, axis=1).astype(jnp.bfloat16)
    out_copies = [pltpu.make_async_copy(pair, out_ref.at[n], out_sem.at[n]) for n in range(copies)]
    for copy in out_copies:
        copy.start()
    for copy in out_copies:
        copy.wait()


def burn_in(place, crowded, rows, more, input_weight, hidden_weight, bias, starts):
    shards, count = starts.shape
    width = input_weight.shape[0]
    hidden_width = hidden_weight.shape[0]
    total = BURN * count
    return pl.pallas_call(
        burn_in_kernel,
        out_shape=jax.ShapeDtypeStruct((shards, 2, count, hidden_width), jnp.bfloat16),
        in_specs=[SMEM, SMEM, HBM, HBM, HBM, HBM, VMEM, VMEM],
        out_specs=HBM,
        scratch_shapes=[
            pltpu.VMEM((shards * ROOM, width), jnp.bfloat16),
            pltpu.VMEM((total, shards * ROOM), jnp.bfloat16),
            pltpu.VMEM((total, width), jnp.bfloat16),
            pltpu.VMEM((total, 4 * hidden_width), jnp.float32),
            pltpu.VMEM(input_weight.shape, jnp.bfloat16),
            pltpu.VMEM(hidden_weight.shape, jnp.bfloat16),
            pltpu.VMEM((2, count, hidden_width), jnp.bfloat16),
            pltpu.SemaphoreType.DMA((4,)),
            pltpu.SemaphoreType.DMA((shards,)),
        ],
        compiler_params=pltpu.CompilerParams(vmem_limit_bytes=58 * MIB),
        cost_estimate=pl.CostEstimate(
            flops=30_000_000_000, bytes_accessed=8 * MIB, transcendentals=0
        ),
        name="burn_in",
    )(place, crowded, rows, more, input_weight, hidden_weight, bias, starts)


def unwritten_kernel(out):
    del out


def unwritten(shape, dtype):
    return pl.pallas_call(
        unwritten_kernel,
        out_shape=jax.ShapeDtypeStruct(shape, dtype),
        out_specs=HBM,
        compiler_params=pltpu.CompilerParams(vmem_limit_bytes=60 * MIB),
        name="unwritten",
    )()


def order_kernel(pairs, rank, raw, out):
    shards, _, count, hidden_width = pairs.shape
    total = shards * count
    column = iota((total, total), 1)
    diagonal = column == iota((total, total), 0)
    rank_of = jnp.sum(jnp.where(diagonal, rank[...].astype(jnp.float32), 0.0), axis=1, keepdims=True)
    raw_of = jnp.sum(jnp.where(diagonal, raw[...], 0.0), axis=1, keepdims=True)
    hot = one_hot((column % count) * shards + column // count == rank_of.astype(jnp.int32))
    for n in range(2):
        state = pairs[:, n].reshape(total, hidden_width)
        out[:, n * hidden_width : (n + 1) * hidden_width] = f32_dot(hot, state).astype(jnp.bfloat16)
    lane = iota((total, 128), 1)
    tail = jnp.where(lane == 0, raw_of, jnp.where(lane == 1, jnp.max(raw_of), 0.0))
    out[:, 2 * hidden_width :] = tail.astype(jnp.bfloat16)


def ordered(pairs, rank, raw):
    total = rank.shape[1]
    return pl.pallas_call(
        order_kernel,
        out_shape=jax.ShapeDtypeStruct((total, 2 * pairs.shape[3] + 128), jnp.bfloat16),
        in_specs=[VMEM] * 3,
        out_specs=VMEM,
        compiler_params=pltpu.CompilerParams(vmem_limit_bytes=8 * MIB),
        cost_estimate=pl.CostEstimate(flops=10**8, bytes_accessed=MIB, transcendentals=0),
        name="learner_order",
    )(pairs, rank, raw)


def weights_kernel(received, out):
    total = received.shape[0]
    raw = received[...].astype(jnp.float32)
    lane = iota(raw.shape, 1)
    peak = jnp.max(jnp.where(lane == 1, raw, 0.0))
    weight = jnp.sum(jnp.where(lane == 0, raw, 0.0), axis=1, keepdims=True) / peak
    weight = jnp.where(iota((total, total), 0) == iota((total, total), 1), weight, 0.0)
    out[...] = jnp.sum(weight, axis=0, keepdims=True).astype(jnp.bfloat16)


def normalized(received):
    total, lanes = received.shape
    return pl.pallas_call(
        weights_kernel,
        grid=(1,),
        out_shape=jax.ShapeDtypeStruct((1, total), jnp.bfloat16),
        in_specs=[pl.BlockSpec((total, 128), lambda n: (0, lanes // 128 - 1))],
        out_specs=pl.BlockSpec((1, total), lambda n: (0, 0)),
        compiler_params=pltpu.CompilerParams(vmem_limit_bytes=4 * MIB),
        name="weights",
    )(received)[0]


def body(
    observations,
    input_weight,
    hidden_weight,
    gate_bias,
    forget_bias,
    episode_ids,
    start_steps,
    priorities,
):
    _, width = observations.shape[1:]
    seq_count = episode_ids.shape[0]
    hidden_width = hidden_weight.shape[0]
    shards = lax.axis_size("tm")
    learners = lax.axis_size(EP)
    place = jnp.stack([lax.axis_index(axis) for axis in ("tm", *EP)]).astype(jnp.int32)
    own_count = seq_count // shards
    per_learner = seq_count // learners

    index = jnp.arange(seq_count, dtype=jnp.int32)
    key = start_steps * seq_count + index
    rank = jnp.sum((key[None, :] < key[:, None]).astype(jnp.int32), axis=1)
    turn = jnp.arange(shards, dtype=jnp.int32)
    dealt = jnp.arange(own_count, dtype=jnp.int32)[None, :] * shards + turn[:, None]
    chosen = rank[None, None, :] == dealt[:, :, None]
    ids = jnp.sum(jnp.where(chosen, episode_ids, 0), axis=2)
    starts = jnp.sum(jnp.where(chosen, start_steps, 0), axis=2)

    def exchanged(base):
        sent, crowded = pack(base, place, ids, starts, observations)
        rows = lax.all_to_all(sent, "tm", split_axis=0, concat_axis=0, tiled=True)
        return rows.reshape(shards * ROOM, width), crowded

    grid = along, across = tuple(lax.axis_size(axis) for axis in EP)

    def hops(n):
        dx, dz = n // across, n % across
        return min(dx, along - dx) + min(dz, across - dz)

    late = [n for n in range(1, learners) if hops(n) == 1]
    order = sorted((n for n in range(1, learners) if n not in late), key=lambda n: (-hops(n), n)) + late
    rows_in, crowded = exchanged(0)
    sent_rows = masked(grid, place, episode_ids, start_steps, observations)
    moved_rows = [sent_rows[0]]
    for n in order:
        ring = [
            (i, (i // across + n // across) % along * across + (i + n) % across)
            for i in range(learners)
        ]
        moved_rows.append(lax.ppermute(sent_rows[n], EP, ring))

    blank = jnp.zeros((hidden_width,), jnp.float32)
    bias = (gate_bias + jnp.concatenate([blank, forget_bias, blank, blank]))[None, :]

    raw_weight = jnp.exp(-IMPORTANCE * jnp.log(priorities.astype(jnp.float32))).astype(jnp.bfloat16)
    raw_row = raw_weight.astype(jnp.float32)[None, :]
    bias, rank_row, raw_row = lax.optimization_barrier((bias, rank[None, :], raw_row))

    rows_in, again = lax.optimization_barrier((rows_in, crowded))
    more = lax.cond(
        again[0] > 0,
        lambda: exchanged(ROOM)[0],
        lambda: unwritten(rows_in.shape, rows_in.dtype),
    )
    pairs = burn_in(place, crowded, rows_in, more, input_weight, hidden_weight, bias, starts)
    pairs = lax.all_to_all(pairs, "tm", split_axis=0, concat_axis=0, tiled=True)
    rows = placed(grid, [0] + order, place, moved_rows)
    both = ordered(pairs, rank_row, raw_row)
    both = both.reshape(learners, per_learner, both.shape[1])
    both = lax.all_to_all(both, EP, split_axis=0, concat_axis=0, tiled=True)
    start_state = both[:, :, : 2 * hidden_width].reshape(seq_count, 2, hidden_width)
    weights = normalized(both.reshape(seq_count, both.shape[2]))
    return (rows, start_state, weights)


def solution(mesh):
    torus = Mesh(mesh.devices.reshape(mesh.shape["tm"], 4, 4), ("tm", "ep_0", "ep_1"))
    return jax.shard_map(
        body,
        mesh=torus,
        in_specs=(P(EP, "tm", None), P(), P(), P(), P(), P(EP), P(EP), P(EP)),
        out_specs=(P(EP, "tm", None), P(EP, None, None), P(EP)),
        check_vma=False,
    )
```

```python
import functools

import jax
import jax.numpy as jnp
from jax import lax
from jax.experimental import pallas as pl
from jax.experimental.pallas import tpu as pltpu
from jax.sharding import Mesh
from jax.sharding import PartitionSpec as P

STEPS = 128
BURN = 40
UNROLL = 80
ROOM = 128
EP = ("ep_0", "ep_1")
IMPORTANCE = 0.6
MIB = 1024 * 1024
SMEM = pl.BlockSpec(memory_space=pltpu.SMEM)
VMEM = pl.BlockSpec(memory_space=pltpu.VMEM)
HBM = pl.BlockSpec(memory_space=pltpu.HBM)


def sigmoid(x):
    return 0.5 * jnp.tanh(0.5 * x) + 0.5


def iota(shape, dim):
    return lax.broadcasted_iota(jnp.int32, shape, dim)


def one_hot(hit):
    return jnp.where(hit, 1.0, 0.0).astype(jnp.bfloat16)


def f32_dot(a, b):
    return jnp.dot(a, b, preferred_element_type=jnp.float32)


def pack_kernel(
    base, place, ids_ref, starts_ref, obs_hbm, out, crowded, dealt, rank_ref, obs, ids_held, ids, rows_of, packed, sem, obs_sem
):
    obs_copy = pltpu.make_async_copy(obs_hbm, obs, obs_sem.at[0])
    obs_copy.start()
    shards, count = dealt.shape
    total = shards * count
    shard_steps = obs.shape[1]
    lanes = count * shard_steps
    row, column = iota((total, total), 0), iota((total, total), 1)

    def upright(values):
        return jnp.sum(jnp.where(row == column, values, 0.0), axis=1, keepdims=True)

    start_row = starts_ref[...].astype(jnp.float32)
    start_column = upright(start_row)
    ahead = (start_row < start_column) | ((start_row == start_column) & (column < row))
    rank_column = jnp.sum(jnp.where(ahead, 1.0, 0.0), axis=1, keepdims=True)
    rank_row = jnp.sum(jnp.where(row == column, rank_column, 0.0), axis=0, keepdims=True)
    rank_ref[...] = rank_row.astype(jnp.int32)
    whole_rank = rank_column.astype(jnp.int32)
    taker = (column % count) * shards + column // count
    ids_row = jnp.where(whole_rank == taker, upright(ids_ref[...].astype(jnp.float32)), 0.0)
    ids_held[...] = jnp.sum(ids_row, axis=0, keepdims=True).astype(jnp.int32)
    ids_copy = pltpu.make_async_copy(ids_held, ids, obs_sem.at[1])
    ids_copy.start()
    to_shard = one_hot(iota((shards, total), 0) == rank_row.astype(jnp.int32) % shards)
    to_place = jnp.where(iota((total, count), 1) == whole_rank // shards, start_column, 0.0)
    dealt_starts = f32_dot(to_shard, to_place.astype(jnp.bfloat16))
    dealt[...] = dealt_starts.astype(jnp.int32)
    spread = one_hot(iota((count, lanes), 1) // shard_steps == iota((count, lanes), 0))
    starts = f32_dot(dealt_starts.astype(jnp.bfloat16), spread).astype(jnp.int32)
    step = place[0] * shard_steps + iota((shards, lanes), 1) % shard_steps
    within = ((step - starts) & (STEPS - 1)) < BURN
    before = one_hot(iota((lanes, lanes), 0) < iota((lanes, lanes), 1))
    slot = f32_dot(one_hot(within), before).astype(jnp.int32) - base
    slot = jnp.where(within, slot, -1)
    most = jnp.zeros((shards, lanes // 2), jnp.float32)
    for shard in range(shards):
        held = ((step + (shard * shard_steps) - starts) & (STEPS - 1)) < BURN
        some = jnp.where(held, 1.0, 0.0)
        most = jnp.maximum(most, f32_dot(some.astype(jnp.bfloat16), jnp.ones((lanes, lanes // 2), jnp.bfloat16)))
    crowded[0] = (jnp.max(most) > ROOM).astype(jnp.int32)
    ids_copy.wait()
    obs_copy.wait()
    copies = [pltpu.make_async_copy(packed.at[k], out.at[k], sem.at[k]) for k in range(shards)]
    for k in range(shards):
        for i in range(count):
            rows_of[k, i * shard_steps : (i + 1) * shard_steps, :] = obs[ids[0, k * count + i]]
        hot = one_hot(iota((ROOM, lanes), 0) == slot[k : k + 1, :])
        packed[k] = f32_dot(hot, rows_of[k]).astype(jnp.bfloat16)
        copies[k].start()
    for copy in copies:
        copy.wait()


def pack(base, place, shards, ids, starts, observations):
    _, shard_steps, width = observations.shape
    total = ids.shape[0]
    count = total // shards
    return pl.pallas_call(
        functools.partial(pack_kernel, base),
        out_shape=(
            jax.ShapeDtypeStruct((shards, ROOM, width), jnp.bfloat16),
            jax.ShapeDtypeStruct((1,), jnp.int32),
            jax.ShapeDtypeStruct((shards, count), jnp.int32),
            jax.ShapeDtypeStruct((1, total), jnp.int32),
        ),
        in_specs=[SMEM, VMEM, VMEM, HBM],
        out_specs=(HBM, SMEM, VMEM, VMEM),
        scratch_shapes=[
            pltpu.VMEM(observations.shape, jnp.bfloat16),
            pltpu.VMEM((1, total), jnp.int32),
            pltpu.SMEM((1, total), jnp.int32),
            pltpu.VMEM((shards, count * shard_steps, width), jnp.bfloat16),
            pltpu.VMEM((shards, ROOM, width), jnp.bfloat16),
            pltpu.SemaphoreType.DMA((shards,)),
            pltpu.SemaphoreType.DMA((2,)),
        ],
        compiler_params=pltpu.CompilerParams(vmem_limit_bytes=58 * MIB),
        cost_estimate=pl.CostEstimate(flops=10**9, bytes_accessed=4 * MIB, transcendentals=0),
        name="pack_rows",
    )(place, ids[None, :], starts[None, :], observations)


def block_at(here, grid, n, sign):
    along, across = grid
    first = lax.rem(here[1] + (along + sign * (n // across)), along)
    return first * across + lax.rem(here[2] + (across + sign * (n % across)), across)


def masked_kernel(grid, place, ids, starts, obs, *refs):
    outs, (held, sem) = refs[:-2], refs[-2:]
    count, shard_steps, width = outs[0].shape
    step = place[0] * shard_steps + iota((shard_steps, width), 0)
    copies = [pltpu.make_async_copy(held.at[n], out, sem.at[n]) for n, out in enumerate(outs)]
    for n in range(len(outs)):
        block = block_at(place, grid, n, 1)
        for i in range(count):
            g = block * count + i
            keep = ((step - starts[g] - BURN) & (STEPS - 1)) < UNROLL
            held[n, i] = jnp.where(keep, obs[ids[g]], jnp.zeros((), jnp.bfloat16))
        copies[n].start()
    for copy in copies:
        copy.wait()


def masked(grid, place, ids, starts, observations):
    _, shard_steps, width = observations.shape
    learners = grid[0] * grid[1]
    block = (ids.shape[0] // learners, shard_steps, width)
    return pl.pallas_call(
        functools.partial(masked_kernel, grid),
        out_shape=[jax.ShapeDtypeStruct(block, jnp.bfloat16)] * learners,
        in_specs=[SMEM, SMEM, SMEM, VMEM],
        out_specs=[HBM] * learners,
        scratch_shapes=[
            pltpu.VMEM((learners, *block), jnp.bfloat16),
            pltpu.SemaphoreType.DMA((learners,)),
        ],
        compiler_params=pltpu.CompilerParams(vmem_limit_bytes=60 * MIB),
        cost_estimate=pl.CostEstimate(flops=10**8, bytes_accessed=6 * MIB, transcendentals=0),
        name="masked_rows",
    )(place, ids, starts, observations)


def place_kernel(grid, sources, place, *refs):
    rows, (out, sem) = refs[: len(sources)], refs[-2:]
    count = rows[0].shape[0]
    copies = [
        pltpu.make_async_copy(
            block, out.at[pl.ds(block_at(place, grid, n, -1) * count, count)], sem.at[m]
        )
        for m, (n, block) in enumerate(zip(sources, rows))
    ]
    for copy in copies:
        copy.start()
    for copy in copies:
        copy.wait()


def placed(grid, sources, place, rows):
    count, shard_steps, width = rows[0].shape
    return pl.pallas_call(
        functools.partial(place_kernel, grid, sources),
        out_shape=jax.ShapeDtypeStruct((grid[0] * grid[1] * count, shard_steps, width), jnp.bfloat16),
        in_specs=[SMEM] + [VMEM] * len(rows),
        out_specs=HBM,
        scratch_shapes=[pltpu.SemaphoreType.DMA((len(rows),))],
        compiler_params=pltpu.CompilerParams(vmem_limit_bytes=8 * MIB),
        cost_estimate=pl.CostEstimate(flops=10**9, bytes_accessed=8 * MIB, transcendentals=0),
        name="place_rows",
    )(place, *rows)


def burn_in_kernel(
    place, crowded, rows_hbm, more_hbm, win_hbm, wh_hbm, bias_ref, starts_ref, out_ref, xs, hot, x, proj, win, wh, pair, sem, out_sem
):
    copies, _, count, hidden_width = out_ref.shape
    shards = starts_ref.shape[0]
    shard_steps = STEPS // shards
    rows_copy = pltpu.make_async_copy(rows_hbm, xs, sem.at[0])
    rows_copy.start()
    win_copy = pltpu.make_async_copy(win_hbm, win, sem.at[2])
    wh_copy = pltpu.make_async_copy(wh_hbm, wh, sem.at[3])
    win_copy.start()
    wh_copy.start()

    mine = jnp.where(iota((shards, count), 0) == place[0], starts_ref[...], 0).astype(jnp.float32)
    mine = jnp.sum(mine, axis=0, keepdims=True)
    diagonal = iota((count, count), 0) == iota((count, count), 1)
    own = jnp.sum(jnp.where(diagonal, mine, 0.0), axis=1, keepdims=True).astype(jnp.int32)
    lane = iota((count, 128), 1)
    first = ((lane - own // shard_steps) & (shards - 1)) * shard_steps - own % shard_steps
    begin = jnp.maximum(first, 0)
    held = jnp.clip(jnp.minimum(first + shard_steps, BURN) - begin, 0, shard_steps)
    earlier = one_hot(iota((count, count), 1) < iota((count, count), 0))
    ahead = f32_dot(earlier, held.astype(jnp.float32).astype(jnp.bfloat16)).astype(jnp.int32)
    slot = iota((count, ROOM), 1)

    def select(base):
        for shard in range(shards):
            at = slice(shard, shard + 1)
            order = slot + base - ahead[:, at]
            step = jnp.where((order >= 0) & (order < held[:, at]), order + begin[:, at], -1)
            for t in range(BURN):
                hot[t * count : (t + 1) * count, shard * ROOM : (shard + 1) * ROOM] = one_hot(step == t)

    select(0)
    rows_copy.wait()
    x[...] = f32_dot(hot[...], xs[...]).astype(jnp.bfloat16)

    @pl.when(crowded[0] > 0)
    def _():
        more_copy = pltpu.make_async_copy(more_hbm, xs, sem.at[1])
        more_copy.start()
        select(ROOM)
        more_copy.wait()
        x[...] += f32_dot(hot[...], xs[...]).astype(jnp.bfloat16)

    win_copy.wait()
    proj[...] = f32_dot(x[...], win[...]) + bias_ref[...]
    wh_copy.wait()
    half = hidden_width // 2

    def step(t, state_pair):
        hiddens, cells = state_pair
        row = pl.ds(pl.multiple_of(t * count, count), count)
        blocks = [[pl.ds(gate * hidden_width + q * half, half) for gate in range(4)] for q in range(2)]
        sums = [[proj[row, block] for block in part] for part in blocks]
        for k in range(2):
            for q in range(2):
                for gate in range(4):
                    weight = wh[k * half : (k + 1) * half, blocks[q][gate]]
                    sums[q][gate] = sums[q][gate] + f32_dot(hiddens[k], weight)
        new_hiddens, new_cells = [], []
        for (ingate, forget, candidate, outgate), cell_state in zip(sums, cells):
            cell_state = sigmoid(forget) * cell_state + sigmoid(ingate) * jnp.tanh(candidate)
            new_cells.append(cell_state)
            new_hiddens.append((sigmoid(outgate) * jnp.tanh(cell_state)).astype(jnp.bfloat16))
        return (tuple(new_hiddens), tuple(new_cells))

    blank = ((jnp.zeros((count, half), jnp.bfloat16),) * 2, (jnp.zeros((count, half), jnp.float32),) * 2)
    hiddens, cells = lax.fori_loop(0, BURN, step, blank, unroll=8)
    pair[0] = jnp.concatenate(hiddens, axis=1)
    pair[1] = jnp.concatenate(cells, axis=1).astype(jnp.bfloat16)
    out_copies = [pltpu.make_async_copy(pair, out_ref.at[n], out_sem.at[n]) for n in range(copies)]
    for copy in out_copies:
        copy.start()
    for copy in out_copies:
        copy.wait()


def burn_in(place, crowded, rows, more, input_weight, hidden_weight, bias, starts):
    shards, count = starts.shape
    width = input_weight.shape[0]
    hidden_width = hidden_weight.shape[0]
    total = BURN * count
    return pl.pallas_call(
        burn_in_kernel,
        out_shape=jax.ShapeDtypeStruct((shards, 2, count, hidden_width), jnp.bfloat16),
        in_specs=[SMEM, SMEM, HBM, HBM, HBM, HBM, VMEM, VMEM],
        out_specs=HBM,
        scratch_shapes=[
            pltpu.VMEM((shards * ROOM, width), jnp.bfloat16),
            pltpu.VMEM((total, shards * ROOM), jnp.bfloat16),
            pltpu.VMEM((total, width), jnp.bfloat16),
            pltpu.VMEM((total, 4 * hidden_width), jnp.float32),
            pltpu.VMEM(input_weight.shape, jnp.bfloat16),
            pltpu.VMEM(hidden_weight.shape, jnp.bfloat16),
            pltpu.VMEM((2, count, hidden_width), jnp.bfloat16),
            pltpu.SemaphoreType.DMA((4,)),
            pltpu.SemaphoreType.DMA((shards,)),
        ],
        compiler_params=pltpu.CompilerParams(vmem_limit_bytes=58 * MIB),
        cost_estimate=pl.CostEstimate(
            flops=30_000_000_000, bytes_accessed=8 * MIB, transcendentals=0
        ),
        name="burn_in",
    )(place, crowded, rows, more, input_weight, hidden_weight, bias, starts)


def unwritten_kernel(out):
    del out


def unwritten(shape, dtype):
    return pl.pallas_call(
        unwritten_kernel,
        out_shape=jax.ShapeDtypeStruct(shape, dtype),
        out_specs=HBM,
        compiler_params=pltpu.CompilerParams(vmem_limit_bytes=60 * MIB),
        name="unwritten",
    )()


def order_kernel(pairs, rank, raw, out):
    shards, _, count, hidden_width = pairs.shape
    total = shards * count
    column = iota((total, total), 1)
    diagonal = column == iota((total, total), 0)
    rank_of = jnp.sum(jnp.where(diagonal, rank[...].astype(jnp.float32), 0.0), axis=1, keepdims=True)
    raw_of = jnp.sum(jnp.where(diagonal, raw[...], 0.0), axis=1, keepdims=True)
    hot = one_hot((column % count) * shards + column // count == rank_of.astype(jnp.int32))
    for n in range(2):
        state = pairs[:, n].reshape(total, hidden_width)
        out[:, n * hidden_width : (n + 1) * hidden_width] = f32_dot(hot, state).astype(jnp.bfloat16)
    lane = iota((total, 128), 1)
    tail = jnp.where(lane == 0, raw_of, jnp.where(lane == 1, jnp.max(raw_of), 0.0))
    out[:, 2 * hidden_width :] = tail.astype(jnp.bfloat16)


def ordered(pairs, rank, raw):
    total = rank.shape[1]
    return pl.pallas_call(
        order_kernel,
        out_shape=jax.ShapeDtypeStruct((total, 2 * pairs.shape[3] + 128), jnp.bfloat16),
        in_specs=[VMEM] * 3,
        out_specs=VMEM,
        compiler_params=pltpu.CompilerParams(vmem_limit_bytes=8 * MIB),
        cost_estimate=pl.CostEstimate(flops=10**8, bytes_accessed=MIB, transcendentals=0),
        name="learner_order",
    )(pairs, rank, raw)


def weights_kernel(received, out):
    total = received.shape[0]
    raw = received[...].astype(jnp.float32)
    lane = iota(raw.shape, 1)
    peak = jnp.max(jnp.where(lane == 1, raw, 0.0))
    weight = jnp.sum(jnp.where(lane == 0, raw, 0.0), axis=1, keepdims=True) / peak
    weight = jnp.where(iota((total, total), 0) == iota((total, total), 1), weight, 0.0)
    out[...] = jnp.sum(weight, axis=0, keepdims=True).astype(jnp.bfloat16)


def normalized(received):
    total, lanes = received.shape
    return pl.pallas_call(
        weights_kernel,
        grid=(1,),
        out_shape=jax.ShapeDtypeStruct((1, total), jnp.bfloat16),
        in_specs=[pl.BlockSpec((total, 128), lambda n: (0, lanes // 128 - 1))],
        out_specs=pl.BlockSpec((1, total), lambda n: (0, 0)),
        compiler_params=pltpu.CompilerParams(vmem_limit_bytes=4 * MIB),
        name="weights",
    )(received)[0]


def body(
    observations,
    input_weight,
    hidden_weight,
    gate_bias,
    forget_bias,
    episode_ids,
    start_steps,
    priorities,
):
    _, width = observations.shape[1:]
    seq_count = episode_ids.shape[0]
    hidden_width = hidden_weight.shape[0]
    shards = lax.axis_size("tm")
    learners = lax.axis_size(EP)
    place = jnp.stack([lax.axis_index(axis) for axis in ("tm", *EP)]).astype(jnp.int32)
    per_learner = seq_count // learners

    def exchanged(base):
        sent, *rest = pack(base, place, shards, episode_ids, start_steps, observations)
        rows = lax.all_to_all(sent, "tm", split_axis=0, concat_axis=0, tiled=True)
        return rows.reshape(shards * ROOM, width), *rest

    grid = along, across = tuple(lax.axis_size(axis) for axis in EP)

    def hops(n):
        dx, dz = n // across, n % across
        return min(dx, along - dx) + min(dz, across - dz)

    late = [n for n in range(1, learners) if hops(n) == 1]
    order = sorted((n for n in range(1, learners) if n not in late), key=lambda n: (-hops(n), n)) + late
    rows_in, crowded, starts, rank_row = exchanged(0)
    sent_rows = masked(grid, place, episode_ids, start_steps, observations)
    moved_rows = [sent_rows[0]]
    for n in order:
        ring = [
            (i, (i // across + n // across) % along * across + (i + n) % across)
            for i in range(learners)
        ]
        moved_rows.append(lax.ppermute(sent_rows[n], EP, ring))

    blank = jnp.zeros((hidden_width,), jnp.float32)
    bias = (gate_bias + jnp.concatenate([blank, forget_bias, blank, blank]))[None, :]

    raw_weight = jnp.exp(-IMPORTANCE * jnp.log(priorities.astype(jnp.float32))).astype(jnp.bfloat16)
    raw_row = raw_weight.astype(jnp.float32)[None, :]
    bias, raw_row = lax.optimization_barrier((bias, raw_row))

    rows_in, again = lax.optimization_barrier((rows_in, crowded))
    more = lax.cond(
        again[0] > 0,
        lambda: exchanged(ROOM)[0],
        lambda: unwritten(rows_in.shape, rows_in.dtype),
    )
    pairs = burn_in(place, crowded, rows_in, more, input_weight, hidden_weight, bias, starts)
    pairs = lax.all_to_all(pairs, "tm", split_axis=0, concat_axis=0, tiled=True)
    rows = placed(grid, [0] + order, place, moved_rows)
    both = ordered(pairs, rank_row, raw_row)
    both = both.reshape(learners, per_learner, both.shape[1])
    both = lax.all_to_all(both, EP, split_axis=0, concat_axis=0, tiled=True)
    start_state = both[:, :, : 2 * hidden_width].reshape(seq_count, 2, hidden_width)
    weights = normalized(both.reshape(seq_count, both.shape[2]))
    return (rows, start_state, weights)


def solution(mesh):
    torus = Mesh(mesh.devices.reshape(mesh.shape["tm"], 4, 4), ("tm", "ep_0", "ep_1"))
    return jax.shard_map(
        body,
        mesh=torus,
        in_specs=(P(EP, "tm", None), P(), P(), P(), P(), P(EP), P(EP), P(EP)),
        out_specs=(P(EP, "tm", None), P(EP, None, None), P(EP)),
        check_vma=False,
    )
```

```python
import functools

import jax
import jax.numpy as jnp
from jax import lax
from jax.experimental import pallas as pl
from jax.experimental.pallas import tpu as pltpu
from jax.sharding import Mesh
from jax.sharding import PartitionSpec as P

STEPS = 128
BURN = 40
UNROLL = 80
ROOM = 128
EP = ("ep_0", "ep_1")
IMPORTANCE = 0.6
MIB = 1024 * 1024
SMEM = pl.BlockSpec(memory_space=pltpu.SMEM)
VMEM = pl.BlockSpec(memory_space=pltpu.VMEM)
HBM = pl.BlockSpec(memory_space=pltpu.HBM)


def sigmoid(x):
    return 0.5 * jnp.tanh(0.5 * x) + 0.5


def iota(shape, dim):
    return lax.broadcasted_iota(jnp.int32, shape, dim)


def one_hot(hit):
    return jnp.where(hit, 1.0, 0.0).astype(jnp.bfloat16)


def f32_dot(a, b):
    return jnp.dot(a, b, preferred_element_type=jnp.float32)


def pack_kernel(
    base, place, ids_ref, starts_ref, obs_hbm, out, crowded, dealt, rank_ref, obs, ids_held, ids, rows_of, packed, sem, obs_sem
):
    obs_copy = pltpu.make_async_copy(obs_hbm, obs, obs_sem.at[0])
    obs_copy.start()
    shards, count = dealt.shape
    total = shards * count
    shard_steps = obs.shape[1]
    lanes = count * shard_steps
    row, column = iota((total, total), 0), iota((total, total), 1)

    def upright(values):
        return jnp.sum(jnp.where(row == column, values, 0.0), axis=1, keepdims=True)

    start_row = starts_ref[...].astype(jnp.float32)
    start_column = upright(start_row)
    ahead = (start_row < start_column) | ((start_row == start_column) & (column < row))
    rank_column = jnp.sum(jnp.where(ahead, 1.0, 0.0), axis=1, keepdims=True)
    rank_row = jnp.sum(jnp.where(row == column, rank_column, 0.0), axis=0, keepdims=True)
    rank_ref[...] = rank_row.astype(jnp.int32)
    whole_rank = rank_column.astype(jnp.int32)
    taker = (column % count) * shards + column // count
    ids_row = jnp.where(whole_rank == taker, upright(ids_ref[...].astype(jnp.float32)), 0.0)
    ids_held[...] = jnp.sum(ids_row, axis=0, keepdims=True).astype(jnp.int32)
    ids_copy = pltpu.make_async_copy(ids_held, ids, obs_sem.at[1])
    ids_copy.start()
    to_shard = one_hot(iota((shards, total), 0) == rank_row.astype(jnp.int32) % shards)
    to_place = jnp.where(iota((total, count), 1) == whole_rank // shards, start_column, 0.0)
    dealt_starts = f32_dot(to_shard, to_place.astype(jnp.bfloat16))
    dealt[...] = dealt_starts.astype(jnp.int32)
    spread = one_hot(iota((count, lanes), 1) // shard_steps == iota((count, lanes), 0))
    starts = f32_dot(dealt_starts.astype(jnp.bfloat16), spread).astype(jnp.int32)
    step = place[0] * shard_steps + iota((shards, lanes), 1) % shard_steps
    within = ((step - starts) & (STEPS - 1)) < BURN
    before = one_hot(iota((lanes, lanes), 0) < iota((lanes, lanes), 1))
    slot = f32_dot(one_hot(within), before).astype(jnp.int32) - base
    slot = jnp.where(within, slot, -1)
    most = jnp.zeros((shards, lanes // 2), jnp.float32)
    for shard in range(shards):
        held = ((step + (shard * shard_steps) - starts) & (STEPS - 1)) < BURN
        some = jnp.where(held, 1.0, 0.0)
        most = jnp.maximum(most, f32_dot(some.astype(jnp.bfloat16), jnp.ones((lanes, lanes // 2), jnp.bfloat16)))
    crowded[0] = (jnp.max(most) > ROOM).astype(jnp.int32)
    ids_copy.wait()
    obs_copy.wait()
    copies = [pltpu.make_async_copy(packed.at[k], out.at[k], sem.at[k]) for k in range(shards)]
    for k in range(shards):
        for i in range(count):
            rows_of[k, i * shard_steps : (i + 1) * shard_steps, :] = obs[ids[0, k * count + i]]
        hot = one_hot(iota((ROOM, lanes), 0) == slot[k : k + 1, :])
        packed[k] = f32_dot(hot, rows_of[k]).astype(jnp.bfloat16)
        copies[k].start()
    for copy in copies:
        copy.wait()


def pack(base, place, shards, ids, starts, observations):
    _, shard_steps, width = observations.shape
    total = ids.shape[0]
    count = total // shards
    return pl.pallas_call(
        functools.partial(pack_kernel, base),
        out_shape=(
            jax.ShapeDtypeStruct((shards, ROOM, width), jnp.bfloat16),
            jax.ShapeDtypeStruct((1,), jnp.int32),
            jax.ShapeDtypeStruct((shards, count), jnp.int32),
            jax.ShapeDtypeStruct((1, total), jnp.int32),
        ),
        in_specs=[SMEM, VMEM, VMEM, HBM],
        out_specs=(HBM, SMEM, VMEM, VMEM),
        scratch_shapes=[
            pltpu.VMEM(observations.shape, jnp.bfloat16),
            pltpu.VMEM((1, total), jnp.int32),
            pltpu.SMEM((1, total), jnp.int32),
            pltpu.VMEM((shards, count * shard_steps, width), jnp.bfloat16),
            pltpu.VMEM((shards, ROOM, width), jnp.bfloat16),
            pltpu.SemaphoreType.DMA((shards,)),
            pltpu.SemaphoreType.DMA((2,)),
        ],
        compiler_params=pltpu.CompilerParams(vmem_limit_bytes=58 * MIB),
        cost_estimate=pl.CostEstimate(flops=10**9, bytes_accessed=4 * MIB, transcendentals=0),
        name="pack_rows",
    )(place, ids[None, :], starts[None, :], observations)


def block_at(here, grid, n, sign):
    along, across = grid
    first = lax.rem(here[1] + (along + sign * (n // across)), along)
    return first * across + lax.rem(here[2] + (across + sign * (n % across)), across)


def masked_kernel(grid, place, ids, starts, obs, *refs):
    outs, (held, sem) = refs[:-2], refs[-2:]
    count, shard_steps, width = outs[0].shape
    step = place[0] * shard_steps + iota((shard_steps, width), 0)
    copies = [pltpu.make_async_copy(held.at[n], out, sem.at[n]) for n, out in enumerate(outs)]
    for n in range(len(outs)):
        block = block_at(place, grid, n, 1)
        for i in range(count):
            g = block * count + i
            keep = ((step - starts[g] - BURN) & (STEPS - 1)) < UNROLL
            held[n, i] = jnp.where(keep, obs[ids[g]], jnp.zeros((), jnp.bfloat16))
        copies[n].start()
    for copy in copies:
        copy.wait()


def masked(grid, place, ids, starts, observations):
    _, shard_steps, width = observations.shape
    learners = grid[0] * grid[1]
    block = (ids.shape[0] // learners, shard_steps, width)
    return pl.pallas_call(
        functools.partial(masked_kernel, grid),
        out_shape=[jax.ShapeDtypeStruct(block, jnp.bfloat16)] * learners,
        in_specs=[SMEM, SMEM, SMEM, VMEM],
        out_specs=[HBM] * learners,
        scratch_shapes=[
            pltpu.VMEM((learners, *block), jnp.bfloat16),
            pltpu.SemaphoreType.DMA((learners,)),
        ],
        compiler_params=pltpu.CompilerParams(vmem_limit_bytes=60 * MIB),
        cost_estimate=pl.CostEstimate(flops=10**8, bytes_accessed=6 * MIB, transcendentals=0),
        name="masked_rows",
    )(place, ids, starts, observations)


def place_kernel(grid, sources, place, *refs):
    rows, (out, sem) = refs[: len(sources)], refs[-2:]
    count = rows[0].shape[0]
    copies = [
        pltpu.make_async_copy(
            block, out.at[pl.ds(block_at(place, grid, n, -1) * count, count)], sem.at[m]
        )
        for m, (n, block) in enumerate(zip(sources, rows))
    ]
    for copy in copies:
        copy.start()
    for copy in copies:
        copy.wait()


def placed(grid, sources, place, rows):
    count, shard_steps, width = rows[0].shape
    return pl.pallas_call(
        functools.partial(place_kernel, grid, sources),
        out_shape=jax.ShapeDtypeStruct((grid[0] * grid[1] * count, shard_steps, width), jnp.bfloat16),
        in_specs=[SMEM] + [VMEM] * len(rows),
        out_specs=HBM,
        scratch_shapes=[pltpu.SemaphoreType.DMA((len(rows),))],
        compiler_params=pltpu.CompilerParams(vmem_limit_bytes=8 * MIB),
        cost_estimate=pl.CostEstimate(flops=10**9, bytes_accessed=8 * MIB, transcendentals=0),
        name="place_rows",
    )(place, *rows)


def burn_in_kernel(
    place, crowded, rows_hbm, more_hbm, win_hbm, wh_hbm, bias_ref, forget_ref, starts_ref, out_ref, xs, hot, x, proj, win, wh, pair, sem, out_sem
):
    copies, _, count, hidden_width = out_ref.shape
    shards = starts_ref.shape[0]
    shard_steps = STEPS // shards

    def fetches(array, to, which):
        pieces = sem.shape[1]
        size = array.shape[0] // pieces
        at = [pl.ds(n * size, size) for n in range(pieces)]
        return [
            pltpu.make_async_copy(array.at[at[n]], to.at[at[n]], sem.at[which, n])
            for n in range(pieces)
        ]

    def start(copies):
        for copy in copies:
            copy.start()

    def wait(copies):
        for copy in copies:
            copy.wait()

    rows_copies = fetches(rows_hbm, xs, 0)
    win_copies = fetches(win_hbm, win, 2)
    wh_copies = fetches(wh_hbm, wh, 3)
    start(rows_copies)
    start(win_copies)
    start(wh_copies)

    mine = jnp.where(iota((shards, count), 0) == place[0], starts_ref[...], 0).astype(jnp.float32)
    mine = jnp.sum(mine, axis=0, keepdims=True)
    diagonal = iota((count, count), 0) == iota((count, count), 1)
    own = jnp.sum(jnp.where(diagonal, mine, 0.0), axis=1, keepdims=True).astype(jnp.int32)
    lane = iota((count, 128), 1)
    first = ((lane - own // shard_steps) & (shards - 1)) * shard_steps - own % shard_steps
    begin = jnp.maximum(first, 0)
    held = jnp.clip(jnp.minimum(first + shard_steps, BURN) - begin, 0, shard_steps)
    earlier = one_hot(iota((count, count), 1) < iota((count, count), 0))
    ahead = f32_dot(earlier, held.astype(jnp.float32).astype(jnp.bfloat16)).astype(jnp.int32)
    slot = iota((count, ROOM), 1)

    def select(base):
        for shard in range(shards):
            at = slice(shard, shard + 1)
            order = slot + base - ahead[:, at]
            step = jnp.where((order >= 0) & (order < held[:, at]), order + begin[:, at], -1)
            for t in range(BURN):
                hot[t * count : (t + 1) * count, shard * ROOM : (shard + 1) * ROOM] = one_hot(step == t)

    select(0)
    wait(rows_copies)
    x[...] = f32_dot(hot[...], xs[...]).astype(jnp.bfloat16)

    @pl.when(crowded[0] > 0)
    def _():
        more_copies = fetches(more_hbm, xs, 1)
        start(more_copies)
        select(ROOM)
        wait(more_copies)
        x[...] += f32_dot(hot[...], xs[...]).astype(jnp.bfloat16)

    wait(win_copies)
    bias = bias_ref[...]
    forget_bias = bias[:, hidden_width : 2 * hidden_width] + forget_ref[...]
    bias = jnp.concatenate([bias[:, :hidden_width], forget_bias, bias[:, 2 * hidden_width :]], axis=1)
    proj[...] = f32_dot(x[...], win[...]) + bias
    wait(wh_copies)
    half = hidden_width // 2

    def step(t, state_pair):
        hiddens, cells = state_pair
        row = pl.ds(pl.multiple_of(t * count, count), count)
        blocks = [[pl.ds(gate * hidden_width + q * half, half) for gate in range(4)] for q in range(2)]
        sums = [[proj[row, block] for block in part] for part in blocks]
        for k in range(2):
            for q in range(2):
                for gate in range(4):
                    weight = wh[k * half : (k + 1) * half, blocks[q][gate]]
                    sums[q][gate] = sums[q][gate] + f32_dot(hiddens[k], weight)
        new_hiddens, new_cells = [], []
        for (ingate, forget, candidate, outgate), cell_state in zip(sums, cells):
            cell_state = sigmoid(forget) * cell_state + sigmoid(ingate) * jnp.tanh(candidate)
            new_cells.append(cell_state)
            new_hiddens.append((sigmoid(outgate) * jnp.tanh(cell_state)).astype(jnp.bfloat16))
        return (tuple(new_hiddens), tuple(new_cells))

    blank = ((jnp.zeros((count, half), jnp.bfloat16),) * 2, (jnp.zeros((count, half), jnp.float32),) * 2)
    hiddens, cells = lax.fori_loop(0, BURN, step, blank, unroll=8)
    pair[0] = jnp.concatenate(hiddens, axis=1)
    pair[1] = jnp.concatenate(cells, axis=1).astype(jnp.bfloat16)
    out_copies = [pltpu.make_async_copy(pair, out_ref.at[n], out_sem.at[n]) for n in range(copies)]
    for copy in out_copies:
        copy.start()
    for copy in out_copies:
        copy.wait()


def burn_in(place, crowded, rows, more, input_weight, hidden_weight, gate_bias, forget_bias, starts):
    shards, count = starts.shape
    width = input_weight.shape[0]
    hidden_width = hidden_weight.shape[0]
    total = BURN * count
    return pl.pallas_call(
        burn_in_kernel,
        out_shape=jax.ShapeDtypeStruct((shards, 2, count, hidden_width), jnp.bfloat16),
        in_specs=[SMEM, SMEM, HBM, HBM, HBM, HBM, VMEM, VMEM, VMEM],
        out_specs=HBM,
        scratch_shapes=[
            pltpu.VMEM((shards * ROOM, width), jnp.bfloat16),
            pltpu.VMEM((total, shards * ROOM), jnp.bfloat16),
            pltpu.VMEM((total, width), jnp.bfloat16),
            pltpu.VMEM((total, 4 * hidden_width), jnp.float32),
            pltpu.VMEM(input_weight.shape, jnp.bfloat16),
            pltpu.VMEM(hidden_weight.shape, jnp.bfloat16),
            pltpu.VMEM((2, count, hidden_width), jnp.bfloat16),
            pltpu.SemaphoreType.DMA((4, 8)),
            pltpu.SemaphoreType.DMA((shards,)),
        ],
        compiler_params=pltpu.CompilerParams(vmem_limit_bytes=58 * MIB),
        cost_estimate=pl.CostEstimate(
            flops=30_000_000_000, bytes_accessed=8 * MIB, transcendentals=0
        ),
        name="burn_in",
    )(place, crowded, rows, more, input_weight, hidden_weight, gate_bias[None, :], forget_bias[None, :], starts)


def unwritten_kernel(out):
    del out


def unwritten(shape, dtype):
    return pl.pallas_call(
        unwritten_kernel,
        out_shape=jax.ShapeDtypeStruct(shape, dtype),
        out_specs=HBM,
        compiler_params=pltpu.CompilerParams(vmem_limit_bytes=60 * MIB),
        name="unwritten",
    )()


def order_kernel(pairs, rank, raw, out):
    shards, _, count, hidden_width = pairs.shape
    total = shards * count
    column = iota((total, total), 1)
    diagonal = column == iota((total, total), 0)
    rank_of = jnp.sum(jnp.where(diagonal, rank[...].astype(jnp.float32), 0.0), axis=1, keepdims=True)
    raw_of = jnp.sum(jnp.where(diagonal, raw[...], 0.0), axis=1, keepdims=True)
    hot = one_hot((column % count) * shards + column // count == rank_of.astype(jnp.int32))
    for n in range(2):
        state = pairs[:, n].reshape(total, hidden_width)
        out[:, n * hidden_width : (n + 1) * hidden_width] = f32_dot(hot, state).astype(jnp.bfloat16)
    lane = iota((total, 128), 1)
    tail = jnp.where(lane == 0, raw_of, jnp.where(lane == 1, jnp.max(raw_of), 0.0))
    out[:, 2 * hidden_width :] = tail.astype(jnp.bfloat16)


def ordered(pairs, rank, raw):
    total = rank.shape[1]
    return pl.pallas_call(
        order_kernel,
        out_shape=jax.ShapeDtypeStruct((total, 2 * pairs.shape[3] + 128), jnp.bfloat16),
        in_specs=[VMEM] * 3,
        out_specs=VMEM,
        compiler_params=pltpu.CompilerParams(vmem_limit_bytes=8 * MIB),
        cost_estimate=pl.CostEstimate(flops=10**8, bytes_accessed=MIB, transcendentals=0),
        name="learner_order",
    )(pairs, rank, raw)


def weights_kernel(received, out):
    total = received.shape[0]
    raw = received[...].astype(jnp.float32)
    lane = iota(raw.shape, 1)
    peak = jnp.max(jnp.where(lane == 1, raw, 0.0))
    weight = jnp.sum(jnp.where(lane == 0, raw, 0.0), axis=1, keepdims=True) / peak
    weight = jnp.where(iota((total, total), 0) == iota((total, total), 1), weight, 0.0)
    out[...] = jnp.sum(weight, axis=0, keepdims=True).astype(jnp.bfloat16)


def normalized(received):
    total, lanes = received.shape
    return pl.pallas_call(
        weights_kernel,
        grid=(1,),
        out_shape=jax.ShapeDtypeStruct((1, total), jnp.bfloat16),
        in_specs=[pl.BlockSpec((total, 128), lambda n: (0, lanes // 128 - 1))],
        out_specs=pl.BlockSpec((1, total), lambda n: (0, 0)),
        compiler_params=pltpu.CompilerParams(vmem_limit_bytes=4 * MIB),
        name="weights",
    )(received)[0]


def body(
    observations,
    input_weight,
    hidden_weight,
    gate_bias,
    forget_bias,
    episode_ids,
    start_steps,
    priorities,
):
    _, width = observations.shape[1:]
    seq_count = episode_ids.shape[0]
    hidden_width = hidden_weight.shape[0]
    shards = lax.axis_size("tm")
    learners = lax.axis_size(EP)
    place = jnp.stack([lax.axis_index(axis) for axis in ("tm", *EP)]).astype(jnp.int32)
    per_learner = seq_count // learners

    def exchanged(base):
        sent, *rest = pack(base, place, shards, episode_ids, start_steps, observations)
        rows = lax.all_to_all(sent, "tm", split_axis=0, concat_axis=0, tiled=True)
        return rows.reshape(shards * ROOM, width), *rest

    grid = along, across = tuple(lax.axis_size(axis) for axis in EP)

    def hops(n):
        dx, dz = n // across, n % across
        return min(dx, along - dx) + min(dz, across - dz)

    late = [n for n in range(1, learners) if hops(n) == 1]
    order = sorted((n for n in range(1, learners) if n not in late), key=lambda n: (-hops(n), n)) + late
    rows_in, crowded, starts, rank_row = exchanged(0)
    sent_rows = masked(grid, place, episode_ids, start_steps, observations)
    moved_rows = [sent_rows[0]]
    for n in order:
        ring = [
            (i, (i // across + n // across) % along * across + (i + n) % across)
            for i in range(learners)
        ]
        moved_rows.append(lax.ppermute(sent_rows[n], EP, ring))

    raw_weight = jnp.exp(-IMPORTANCE * jnp.log(priorities.astype(jnp.float32))).astype(jnp.bfloat16)
    raw_row = raw_weight.astype(jnp.float32)[None, :]

    rows_in, again = lax.optimization_barrier((rows_in, crowded))
    more = lax.cond(
        again[0] > 0,
        lambda: exchanged(ROOM)[0],
        lambda: unwritten(rows_in.shape, rows_in.dtype),
    )
    pairs = burn_in(
        place, crowded, rows_in, more, input_weight, hidden_weight, gate_bias, forget_bias, starts
    )
    pairs = lax.all_to_all(pairs, "tm", split_axis=0, concat_axis=0, tiled=True)
    rows = placed(grid, [0] + order, place, moved_rows)
    both = ordered(pairs, rank_row, raw_row)
    both = both.reshape(learners, per_learner, both.shape[1])
    both = lax.all_to_all(both, EP, split_axis=0, concat_axis=0, tiled=True)
    start_state = both[:, :, : 2 * hidden_width].reshape(seq_count, 2, hidden_width)
    weights = normalized(both.reshape(seq_count, both.shape[2]))
    return (rows, start_state, weights)


def solution(mesh):
    torus = Mesh(mesh.devices.reshape(mesh.shape["tm"], 4, 4), ("tm", "ep_0", "ep_1"))
    return jax.shard_map(
        body,
        mesh=torus,
        in_specs=(P(EP, "tm", None), P(), P(), P(), P(), P(EP), P(EP), P(EP)),
        out_specs=(P(EP, "tm", None), P(EP, None, None), P(EP)),
        check_vma=False,
    )
```

```python
import functools

import jax
import jax.numpy as jnp
from jax import lax
from jax.experimental import pallas as pl
from jax.experimental.pallas import tpu as pltpu
from jax.sharding import Mesh
from jax.sharding import PartitionSpec as P

STEPS = 128
BURN = 40
UNROLL = 80
ROOM = 128
EP = ("ep_0", "ep_1")
IMPORTANCE = 0.6
MIB = 1024 * 1024
SMEM = pl.BlockSpec(memory_space=pltpu.SMEM)
VMEM = pl.BlockSpec(memory_space=pltpu.VMEM)
HBM = pl.BlockSpec(memory_space=pltpu.HBM)


def sigmoid(x):
    return 0.5 * jnp.tanh(0.5 * x) + 0.5


def iota(shape, dim):
    return lax.broadcasted_iota(jnp.int32, shape, dim)


def one_hot(hit):
    return jnp.where(hit, 1.0, 0.0).astype(jnp.bfloat16)


def f32_dot(a, b):
    return jnp.dot(a, b, preferred_element_type=jnp.float32)


def pack_kernel(
    base, place, ids_ref, starts_ref, obs_hbm, out, crowded, dealt, rank_ref, obs, ids_held, ids, rows_of, packed, sem, obs_sem
):
    piece = obs.shape[0] // 8
    pieces = [pl.ds(n * piece, piece) for n in range(8)]
    obs_copies = [
        pltpu.make_async_copy(obs_hbm.at[at], obs.at[at], obs_sem.at[n]) for n, at in enumerate(pieces)
    ]
    for copy in obs_copies:
        copy.start()
    shards, count = dealt.shape
    total = shards * count
    shard_steps = obs.shape[1]
    lanes = count * shard_steps
    row, column = iota((total, total), 0), iota((total, total), 1)

    def upright(values):
        return jnp.sum(jnp.where(row == column, values, 0.0), axis=1, keepdims=True)

    start_row = starts_ref[...].astype(jnp.float32)
    start_column = upright(start_row)
    ahead = (start_row < start_column) | ((start_row == start_column) & (column < row))
    rank_column = jnp.sum(jnp.where(ahead, 1.0, 0.0), axis=1, keepdims=True)
    rank_row = jnp.sum(jnp.where(row == column, rank_column, 0.0), axis=0, keepdims=True)
    rank_ref[...] = rank_row.astype(jnp.int32)
    whole_rank = rank_column.astype(jnp.int32)
    taker = (column % count) * shards + column // count
    ids_row = jnp.where(whole_rank == taker, upright(ids_ref[...].astype(jnp.float32)), 0.0)
    ids_held[...] = jnp.sum(ids_row, axis=0, keepdims=True).astype(jnp.int32)
    ids_copy = pltpu.make_async_copy(ids_held, ids, obs_sem.at[8])
    ids_copy.start()
    to_shard = one_hot(iota((shards, total), 0) == rank_row.astype(jnp.int32) % shards)
    to_place = jnp.where(iota((total, count), 1) == whole_rank // shards, start_column, 0.0)
    dealt_starts = f32_dot(to_shard, to_place.astype(jnp.bfloat16))
    dealt[...] = dealt_starts.astype(jnp.int32)
    spread = one_hot(iota((count, lanes), 1) // shard_steps == iota((count, lanes), 0))
    starts = f32_dot(dealt_starts.astype(jnp.bfloat16), spread).astype(jnp.int32)
    step = place[0] * shard_steps + iota((shards, lanes), 1) % shard_steps
    within = ((step - starts) & (STEPS - 1)) < BURN
    before = one_hot(iota((lanes, lanes), 0) < iota((lanes, lanes), 1))
    slot = f32_dot(one_hot(within), before).astype(jnp.int32) - base
    slot = jnp.where(within, slot, -1)
    most = jnp.zeros((shards, lanes // 2), jnp.float32)
    for shard in range(shards):
        held = ((step + (shard * shard_steps) - starts) & (STEPS - 1)) < BURN
        some = jnp.where(held, 1.0, 0.0)
        most = jnp.maximum(most, f32_dot(some.astype(jnp.bfloat16), jnp.ones((lanes, lanes // 2), jnp.bfloat16)))
    crowded[0] = (jnp.max(most) > ROOM).astype(jnp.int32)
    ids_copy.wait()
    for copy in obs_copies:
        copy.wait()
    copies = [pltpu.make_async_copy(packed.at[k], out.at[k], sem.at[k]) for k in range(shards)]
    for k in range(shards):
        for i in range(count):
            rows_of[k, i * shard_steps : (i + 1) * shard_steps, :] = obs[ids[0, k * count + i]]
        hot = one_hot(iota((ROOM, lanes), 0) == slot[k : k + 1, :])
        packed[k] = f32_dot(hot, rows_of[k]).astype(jnp.bfloat16)
        copies[k].start()
    for copy in copies:
        copy.wait()


def pack(base, place, shards, ids, starts, observations):
    _, shard_steps, width = observations.shape
    total = ids.shape[0]
    count = total // shards
    return pl.pallas_call(
        functools.partial(pack_kernel, base),
        out_shape=(
            jax.ShapeDtypeStruct((shards, ROOM, width), jnp.bfloat16),
            jax.ShapeDtypeStruct((1,), jnp.int32),
            jax.ShapeDtypeStruct((shards, count), jnp.int32),
            jax.ShapeDtypeStruct((1, total), jnp.int32),
        ),
        in_specs=[SMEM, VMEM, VMEM, HBM],
        out_specs=(HBM, SMEM, VMEM, VMEM),
        scratch_shapes=[
            pltpu.VMEM(observations.shape, jnp.bfloat16),
            pltpu.VMEM((1, total), jnp.int32),
            pltpu.SMEM((1, total), jnp.int32),
            pltpu.VMEM((shards, count * shard_steps, width), jnp.bfloat16),
            pltpu.VMEM((shards, ROOM, width), jnp.bfloat16),
            pltpu.SemaphoreType.DMA((shards,)),
            pltpu.SemaphoreType.DMA((9,)),
        ],
        compiler_params=pltpu.CompilerParams(vmem_limit_bytes=58 * MIB),
        cost_estimate=pl.CostEstimate(flops=10**9, bytes_accessed=4 * MIB, transcendentals=0),
        name="pack_rows",
    )(place, ids[None, :], starts[None, :], observations)


def block_at(here, grid, n, sign):
    along, across = grid
    first = lax.rem(here[1] + (along + sign * (n // across)), along)
    return first * across + lax.rem(here[2] + (across + sign * (n % across)), across)


def masked_kernel(grid, place, ids, starts, obs, *refs):
    outs, (held, sem) = refs[:-2], refs[-2:]
    count, shard_steps, width = outs[0].shape
    step = place[0] * shard_steps + iota((shard_steps, width), 0)
    copies = [pltpu.make_async_copy(held.at[n], out, sem.at[n]) for n, out in enumerate(outs)]
    for n in range(len(outs)):
        block = block_at(place, grid, n, 1)
        for i in range(count):
            g = block * count + i
            keep = ((step - starts[g] - BURN) & (STEPS - 1)) < UNROLL
            held[n, i] = jnp.where(keep, obs[ids[g]], jnp.zeros((), jnp.bfloat16))
        copies[n].start()
    for copy in copies:
        copy.wait()


def masked(grid, place, ids, starts, observations):
    _, shard_steps, width = observations.shape
    learners = grid[0] * grid[1]
    block = (ids.shape[0] // learners, shard_steps, width)
    return pl.pallas_call(
        functools.partial(masked_kernel, grid),
        out_shape=[jax.ShapeDtypeStruct(block, jnp.bfloat16)] * learners,
        in_specs=[SMEM, SMEM, SMEM, VMEM],
        out_specs=[HBM] * learners,
        scratch_shapes=[
            pltpu.VMEM((learners, *block), jnp.bfloat16),
            pltpu.SemaphoreType.DMA((learners,)),
        ],
        compiler_params=pltpu.CompilerParams(vmem_limit_bytes=60 * MIB),
        cost_estimate=pl.CostEstimate(flops=10**8, bytes_accessed=6 * MIB, transcendentals=0),
        name="masked_rows",
    )(place, ids, starts, observations)


def place_kernel(grid, sources, place, *refs):
    rows, (out, sem) = refs[: len(sources)], refs[-2:]
    count = rows[0].shape[0]
    copies = [
        pltpu.make_async_copy(
            block, out.at[pl.ds(block_at(place, grid, n, -1) * count, count)], sem.at[m]
        )
        for m, (n, block) in enumerate(zip(sources, rows))
    ]
    for copy in copies:
        copy.start()
    for copy in copies:
        copy.wait()


def placed(grid, sources, place, rows):
    count, shard_steps, width = rows[0].shape
    return pl.pallas_call(
        functools.partial(place_kernel, grid, sources),
        out_shape=jax.ShapeDtypeStruct((grid[0] * grid[1] * count, shard_steps, width), jnp.bfloat16),
        in_specs=[SMEM] + [VMEM] * len(rows),
        out_specs=HBM,
        scratch_shapes=[pltpu.SemaphoreType.DMA((len(rows),))],
        compiler_params=pltpu.CompilerParams(vmem_limit_bytes=8 * MIB),
        cost_estimate=pl.CostEstimate(flops=10**9, bytes_accessed=8 * MIB, transcendentals=0),
        name="place_rows",
    )(place, *rows)


def burn_in_kernel(
    place, crowded, rows_hbm, more_hbm, win_hbm, wh_hbm, bias_ref, forget_ref, starts_ref, out_ref, xs, hot, x, proj, win, wh, pair, sem, out_sem
):
    copies, _, count, hidden_width = out_ref.shape
    shards = starts_ref.shape[0]
    shard_steps = STEPS // shards

    def fetches(array, to, which):
        pieces = sem.shape[1]
        size = array.shape[0] // pieces
        at = [pl.ds(n * size, size) for n in range(pieces)]
        return [
            pltpu.make_async_copy(array.at[at[n]], to.at[at[n]], sem.at[which, n])
            for n in range(pieces)
        ]

    def start(copies):
        for copy in copies:
            copy.start()

    def wait(copies):
        for copy in copies:
            copy.wait()

    rows_copies = fetches(rows_hbm, xs, 0)
    win_copies = fetches(win_hbm, win, 2)
    wh_copies = fetches(wh_hbm, wh, 3)
    start(rows_copies)
    start(win_copies)
    start(wh_copies)

    mine = jnp.where(iota((shards, count), 0) == place[0], starts_ref[...], 0).astype(jnp.float32)
    mine = jnp.sum(mine, axis=0, keepdims=True)
    diagonal = iota((count, count), 0) == iota((count, count), 1)
    own = jnp.sum(jnp.where(diagonal, mine, 0.0), axis=1, keepdims=True).astype(jnp.int32)
    lane = iota((count, 128), 1)
    first = ((lane - own // shard_steps) & (shards - 1)) * shard_steps - own % shard_steps
    begin = jnp.maximum(first, 0)
    held = jnp.clip(jnp.minimum(first + shard_steps, BURN) - begin, 0, shard_steps)
    earlier = one_hot(iota((count, count), 1) < iota((count, count), 0))
    ahead = f32_dot(earlier, held.astype(jnp.float32).astype(jnp.bfloat16)).astype(jnp.int32)
    slot = iota((count, ROOM), 1)

    def select(base):
        for shard in range(shards):
            at = slice(shard, shard + 1)
            order = slot + base - ahead[:, at]
            step = jnp.where((order >= 0) & (order < held[:, at]), order + begin[:, at], -1)
            for t in range(BURN):
                hot[t * count : (t + 1) * count, shard * ROOM : (shard + 1) * ROOM] = one_hot(step == t)

    select(0)
    wait(rows_copies)
    x[...] = f32_dot(hot[...], xs[...]).astype(jnp.bfloat16)

    @pl.when(crowded[0] > 0)
    def _():
        more_copies = fetches(more_hbm, xs, 1)
        start(more_copies)
        select(ROOM)
        wait(more_copies)
        x[...] += f32_dot(hot[...], xs[...]).astype(jnp.bfloat16)

    wait(win_copies)
    bias = bias_ref[...]
    forget_bias = bias[:, hidden_width : 2 * hidden_width] + forget_ref[...]
    bias = jnp.concatenate([bias[:, :hidden_width], forget_bias, bias[:, 2 * hidden_width :]], axis=1)
    proj[...] = f32_dot(x[...], win[...]) + bias
    wait(wh_copies)
    half = hidden_width // 2

    def step(t, state_pair):
        hiddens, cells = state_pair
        row = pl.ds(pl.multiple_of(t * count, count), count)
        blocks = [[pl.ds(gate * hidden_width + q * half, half) for gate in range(4)] for q in range(2)]
        sums = [[proj[row, block] for block in part] for part in blocks]
        for k in range(2):
            for q in range(2):
                for gate in range(4):
                    weight = wh[k * half : (k + 1) * half, blocks[q][gate]]
                    sums[q][gate] = sums[q][gate] + f32_dot(hiddens[k], weight)
        new_hiddens, new_cells = [], []
        for (ingate, forget, candidate, outgate), cell_state in zip(sums, cells):
            cell_state = sigmoid(forget) * cell_state + sigmoid(ingate) * jnp.tanh(candidate)
            new_cells.append(cell_state)
            new_hiddens.append((sigmoid(outgate) * jnp.tanh(cell_state)).astype(jnp.bfloat16))
        return (tuple(new_hiddens), tuple(new_cells))

    blank = ((jnp.zeros((count, half), jnp.bfloat16),) * 2, (jnp.zeros((count, half), jnp.float32),) * 2)
    hiddens, cells = lax.fori_loop(0, BURN, step, blank, unroll=8)
    pair[0] = jnp.concatenate(hiddens, axis=1)
    pair[1] = jnp.concatenate(cells, axis=1).astype(jnp.bfloat16)
    out_copies = [pltpu.make_async_copy(pair, out_ref.at[n], out_sem.at[n]) for n in range(copies)]
    for copy in out_copies:
        copy.start()
    for copy in out_copies:
        copy.wait()


def burn_in(place, crowded, rows, more, input_weight, hidden_weight, gate_bias, forget_bias, starts):
    shards, count = starts.shape
    width = input_weight.shape[0]
    hidden_width = hidden_weight.shape[0]
    total = BURN * count
    return pl.pallas_call(
        burn_in_kernel,
        out_shape=jax.ShapeDtypeStruct((shards, 2, count, hidden_width), jnp.bfloat16),
        in_specs=[SMEM, SMEM, HBM, HBM, HBM, HBM, VMEM, VMEM, VMEM],
        out_specs=HBM,
        scratch_shapes=[
            pltpu.VMEM((shards * ROOM, width), jnp.bfloat16),
            pltpu.VMEM((total, shards * ROOM), jnp.bfloat16),
            pltpu.VMEM((total, width), jnp.bfloat16),
            pltpu.VMEM((total, 4 * hidden_width), jnp.float32),
            pltpu.VMEM(input_weight.shape, jnp.bfloat16),
            pltpu.VMEM(hidden_weight.shape, jnp.bfloat16),
            pltpu.VMEM((2, count, hidden_width), jnp.bfloat16),
            pltpu.SemaphoreType.DMA((4, 8)),
            pltpu.SemaphoreType.DMA((shards,)),
        ],
        compiler_params=pltpu.CompilerParams(vmem_limit_bytes=58 * MIB),
        cost_estimate=pl.CostEstimate(
            flops=30_000_000_000, bytes_accessed=8 * MIB, transcendentals=0
        ),
        name="burn_in",
    )(place, crowded, rows, more, input_weight, hidden_weight, gate_bias[None, :], forget_bias[None, :], starts)


def unwritten_kernel(out):
    del out


def unwritten(shape, dtype):
    return pl.pallas_call(
        unwritten_kernel,
        out_shape=jax.ShapeDtypeStruct(shape, dtype),
        out_specs=HBM,
        compiler_params=pltpu.CompilerParams(vmem_limit_bytes=60 * MIB),
        name="unwritten",
    )()


def order_kernel(pairs, rank, raw, out):
    shards, _, count, hidden_width = pairs.shape
    total = shards * count
    column = iota((total, total), 1)
    diagonal = column == iota((total, total), 0)
    rank_of = jnp.sum(jnp.where(diagonal, rank[...].astype(jnp.float32), 0.0), axis=1, keepdims=True)
    raw_of = jnp.sum(jnp.where(diagonal, raw[...], 0.0), axis=1, keepdims=True)
    hot = one_hot((column % count) * shards + column // count == rank_of.astype(jnp.int32))
    for n in range(2):
        state = pairs[:, n].reshape(total, hidden_width)
        out[:, n * hidden_width : (n + 1) * hidden_width] = f32_dot(hot, state).astype(jnp.bfloat16)
    lane = iota((total, 128), 1)
    tail = jnp.where(lane == 0, raw_of, jnp.where(lane == 1, jnp.max(raw_of), 0.0))
    out[:, 2 * hidden_width :] = tail.astype(jnp.bfloat16)


def ordered(pairs, rank, raw):
    total = rank.shape[1]
    return pl.pallas_call(
        order_kernel,
        out_shape=jax.ShapeDtypeStruct((total, 2 * pairs.shape[3] + 128), jnp.bfloat16),
        in_specs=[VMEM] * 3,
        out_specs=VMEM,
        compiler_params=pltpu.CompilerParams(vmem_limit_bytes=8 * MIB),
        cost_estimate=pl.CostEstimate(flops=10**8, bytes_accessed=MIB, transcendentals=0),
        name="learner_order",
    )(pairs, rank, raw)


def weights_kernel(received, out):
    total = received.shape[0]
    raw = received[...].astype(jnp.float32)
    lane = iota(raw.shape, 1)
    peak = jnp.max(jnp.where(lane == 1, raw, 0.0))
    weight = jnp.sum(jnp.where(lane == 0, raw, 0.0), axis=1, keepdims=True) / peak
    weight = jnp.where(iota((total, total), 0) == iota((total, total), 1), weight, 0.0)
    out[...] = jnp.sum(weight, axis=0, keepdims=True).astype(jnp.bfloat16)


def normalized(received):
    total, lanes = received.shape
    return pl.pallas_call(
        weights_kernel,
        grid=(1,),
        out_shape=jax.ShapeDtypeStruct((1, total), jnp.bfloat16),
        in_specs=[pl.BlockSpec((total, 128), lambda n: (0, lanes // 128 - 1))],
        out_specs=pl.BlockSpec((1, total), lambda n: (0, 0)),
        compiler_params=pltpu.CompilerParams(vmem_limit_bytes=4 * MIB),
        name="weights",
    )(received)[0]


def body(
    observations,
    input_weight,
    hidden_weight,
    gate_bias,
    forget_bias,
    episode_ids,
    start_steps,
    priorities,
):
    _, width = observations.shape[1:]
    seq_count = episode_ids.shape[0]
    hidden_width = hidden_weight.shape[0]
    shards = lax.axis_size("tm")
    learners = lax.axis_size(EP)
    place = jnp.stack([lax.axis_index(axis) for axis in ("tm", *EP)]).astype(jnp.int32)
    per_learner = seq_count // learners

    def exchanged(base):
        sent, *rest = pack(base, place, shards, episode_ids, start_steps, observations)
        rows = lax.all_to_all(sent, "tm", split_axis=0, concat_axis=0, tiled=True)
        return rows.reshape(shards * ROOM, width), *rest

    grid = along, across = tuple(lax.axis_size(axis) for axis in EP)

    def hops(n):
        dx, dz = n // across, n % across
        return min(dx, along - dx) + min(dz, across - dz)

    late = [n for n in range(1, learners) if hops(n) == 1]
    order = sorted((n for n in range(1, learners) if n not in late), key=lambda n: (-hops(n), n)) + late
    rows_in, crowded, starts, rank_row = exchanged(0)
    sent_rows = masked(grid, place, episode_ids, start_steps, observations)
    moved_rows = [sent_rows[0]]
    for n in order:
        ring = [
            (i, (i // across + n // across) % along * across + (i + n) % across)
            for i in range(learners)
        ]
        moved_rows.append(lax.ppermute(sent_rows[n], EP, ring))

    raw_weight = jnp.exp(-IMPORTANCE * jnp.log(priorities.astype(jnp.float32))).astype(jnp.bfloat16)
    raw_row = raw_weight.astype(jnp.float32)[None, :]

    rows_in, again = lax.optimization_barrier((rows_in, crowded))
    more = lax.cond(
        again[0] > 0,
        lambda: exchanged(ROOM)[0],
        lambda: unwritten(rows_in.shape, rows_in.dtype),
    )
    pairs = burn_in(
        place, crowded, rows_in, more, input_weight, hidden_weight, gate_bias, forget_bias, starts
    )
    pairs = lax.all_to_all(pairs, "tm", split_axis=0, concat_axis=0, tiled=True)
    rows = placed(grid, [0] + order, place, moved_rows)
    both = ordered(pairs, rank_row, raw_row)
    both = both.reshape(learners, per_learner, both.shape[1])
    both = lax.all_to_all(both, EP, split_axis=0, concat_axis=0, tiled=True)
    start_state = both[:, :, : 2 * hidden_width].reshape(seq_count, 2, hidden_width)
    weights = normalized(both.reshape(seq_count, both.shape[2]))
    return (rows, start_state, weights)


def solution(mesh):
    torus = Mesh(mesh.devices.reshape(mesh.shape["tm"], 4, 4), ("tm", "ep_0", "ep_1"))
    return jax.shard_map(
        body,
        mesh=torus,
        in_specs=(P(EP, "tm", None), P(), P(), P(), P(), P(EP), P(EP), P(EP)),
        out_specs=(P(EP, "tm", None), P(EP, None, None), P(EP)),
        check_vma=False,
    )
```
